256 devices in a mesh: expert: 8 (over x, y_lo), tensor: 16 (over y_hi, z), dp: 2 (over core).
Axes of the slice: x: 4, y: 4 (y_hi: 2, y_lo: 2; y = y_hi * 2 + y_lo), z: 8, core: 2. Of those that a mesh axis runs over, the one named last changes fastest.
Arguments:
- x_real: bfloat16 [4096, 2048], P(('expert', 'dp'), 'tensor'), may hold values from -6 to 6
- routes_real: int32 [4096, 2], P(('expert', 'dp')), may hold values from 0 to 7, all different within a row; in each aligned block of 256 rows (0 to 255, 256 to 511, ...) at most 128 rows name the same one
- gates_real: float32 [4096, 2], P(('expert', 'dp')), may hold values from 0.2 to 1
- up_real: bfloat16 [8, 2048, 8192], P('expert', None, 'tensor'), may hold values from -0.125 to 0.125
- down_real: bfloat16 [8, 8192, 2048], P('expert', 'tensor'), may hold values from -0.0625 to 0.0625
- x_fake: bfloat16 [4096, 2048], P(('expert', 'dp'), 'tensor'), may hold values from -6 to 6
- routes_fake: int32 [4096, 2], P(('expert', 'dp')), may hold values from 0 to 7, all different within a row; in each aligned block of 256 rows (0 to 255, 256 to 511, ...) at most 128 rows name the same one
- gates_fake: float32 [4096, 2], P(('expert', 'dp')), may hold values from 0.2 to 1
- cotangent: bfloat16 [4096, 2048], P(('expert', 'dp'), 'tensor'), may hold values from -6 to 6
- up_fake: bfloat16 [8, 2048, 8192], P('expert', None, 'tensor'), may hold values from -0.125 to 0.125
- down_fake: bfloat16 [8, 8192, 2048], P('expert', 'tensor'), may hold values from -0.0625 to 0.0625
Outputs:
- real_out: bfloat16 [4096, 2048], P(('expert', 'dp'), 'tensor')
- grad_up: bfloat16 [8, 2048, 8192], P('expert', 'dp', 'tensor')
- grad_down: bfloat16 [8, 8192, 2048], P('expert', 'tensor', 'dp')
The draws below stay inside these ranges and needn't reach their ends.
Inputs may be any that keep to these rules, and one draw needn't show every extreme that they name: `routes_real`: each row names 2 different experts. In the 256 rows of one index of expert and dp no expert is named more than 128 times, and that bound is reached. `routes_fake`: each row names 2 different experts. In the 256 rows of one index of expert and dp no expert is named more than 128 times, and that bound is reached.
All inputs are finite; a program needn't handle non-finite values.
Results may differ from the reference program's by a relative error of at most 0.0058.
Values may be sent and summed in bfloat16 or wider, within the bound.
A program may use at most 128 MiB of HBM per device.

```python
import math
import jax
import jax.numpy as jnp
import numpy as np
from jax import lax

D = 2048
FF = 8192
TOP = 2
TOK_DEV = 256
CAP = 128
EXPERTS = 8
TOKENS = 4096


def block_scale(rng, shape, split, smallest, high):
    loudness = 1.0
    for axis_at, blocks in split:
        draws = jax.random.uniform(jax.random.fold_in(jax.random.fold_in(rng, 6), axis_at), (blocks,), jnp.float32, smallest / len(split), high / len(split))
        loudness = loudness * jnp.repeat(jnp.exp(draws), shape[axis_at] // blocks).reshape((-1,) + (1,) * (len(shape) - 1 - axis_at))
    return loudness


def deal_out(stream_key, own, number, rows, count, top, reach, skew):
    order = jax.random.permutation(stream_key, count)
    crowded, usual = load_shares(count, rows * top, reach, skew, True), load_shares(count, rows * top, reach, skew, False)
    places = jnp.arange(count)

    def named(tallies, turn):
        used = int((tallies > 0).sum())
        fixed = max(1, used // 4)
        shifted = fixed + (places - fixed + turn * (used - fixed)) % max(1, count - fixed)
        return jnp.zeros((count,), jnp.int32).at[order[jnp.where(places < fixed, places, shifted)]].set(jnp.asarray(tallies, jnp.int32))

    tallies = jnp.where(number % 4 == 0, named(crowded, number // 4), named(usual, number - number // 4 - 1))
    mixed = jax.random.permutation(jax.random.fold_in(own, 3), count)
    source_of, receiver = mixed[0:count // 2 * 2:2], mixed[1:count // 2 * 2:2]
    margin = jnp.minimum(tallies[source_of] - 1, reach - tallies[receiver]) // 2
    margin = jnp.where((source_of == order[0]) | (receiver == order[0]) | (tallies[receiver] == 0), 0, jnp.maximum(margin, 0))
    shifted = jax.random.randint(jax.random.fold_in(own, 4), (count // 2,), 0, 1 << 20) % (margin + 1)
    tallies = tallies.at[source_of].add(-shifted).at[receiver].add(shifted)
    members = jnp.searchsorted(jnp.cumsum(tallies), jnp.arange(rows * top), side="right").astype(jnp.int32)
    table = members.reshape(top, rows).T
    table = table[jax.random.permutation(jax.random.fold_in(own, 1), rows)]
    turn = jax.random.randint(jax.random.fold_in(own, 2), (rows, 1), 0, top)
    return jnp.take_along_axis(table, (jnp.arange(top)[None, :] + turn) % top, axis=1)


def load_shares(number_of, total, limit, lean, full):
    weights = [(1 << 20) // math.isqrt(rank ** lean) + 1 for rank in range(1, number_of + 1)]
    largest = limit if full else min(limit, max(-(-total // number_of), total * weights[0] // sum(weights)))
    least = 1 if total - largest >= number_of - 1 else 0
    holding, spare = [largest] + [least] * (number_of - 1), total - largest - least * (number_of - 1)
    while spare > 0:
        free = [i for i in range(1, number_of) if holding[i] < largest] or [i for i in range(1, number_of) if holding[i] < limit]
        mass, left = sum([weights[i] for i in free]), spare
        for i in free:
            addition = min(limit - holding[i], max(1, left * weights[i] // mass), spare)
            holding[i] = holding[i] + addition
            spare = spare - addition
    return np.array(holding)


def scatter_about(rng, extent, deviation, bound, shards=(), kind=jnp.bfloat16):
    array = jax.random.normal(rng, extent, jnp.float32) * deviation
    if len(shards) > 0:
        array = block_scale(rng, extent, shards, -0.22, 0.18) * array
    return jnp.clip(array, min=-bound, max=bound).astype(kind)


def setup_inputs(seed: int = 0) -> dict:
    seeds = jax.random.split(jax.random.key(seed), 12)
    x_real = scatter_about(seeds[0], (TOKENS, D), 1.0, 6.0, ((0, 16), (1, 16)))
    routes_real_keys = jax.random.split(jax.random.fold_in(seeds[1], 1), TOKENS // TOK_DEV)
    routes_real_turns = jax.random.permutation(jax.random.fold_in(seeds[1], 3), TOKENS // TOK_DEV)
    routes_real = jax.vmap(lambda own, number: deal_out(jax.random.fold_in(seeds[1], 2), own, number, TOK_DEV, EXPERTS, TOP, CAP, 2))(routes_real_keys, routes_real_turns).reshape((TOKENS, TOP))
    gates_real = jnp.clip(jnp.exp(math.log(1.0) - 1.609438 * jax.random.uniform(seeds[2], (TOKENS, TOP), jnp.float32) ** block_scale(seeds[2], (TOKENS, TOP), ((0, 16),), -0.2, 0.2)), 0.2, 1.0)
    up_real = scatter_about(seeds[3], (EXPERTS, D, FF), D ** -0.5, 0.125, ((0, 8), (2, 16)))
    down_real = scatter_about(seeds[4], (EXPERTS, FF, D), FF ** -0.5, 0.0625, ((0, 8), (1, 16)))
    x_fake = scatter_about(seeds[5], (TOKENS, D), 1.0, 6.0, ((0, 16), (1, 16)))
    routes_fake_keys = jax.random.split(jax.random.fold_in(seeds[6], 1), TOKENS // TOK_DEV)
    routes_fake_turns = jax.random.permutation(jax.random.fold_in(seeds[6], 3), TOKENS // TOK_DEV)
    routes_fake = jax.vmap(lambda own, number: deal_out(jax.random.fold_in(seeds[6], 2), own, number, TOK_DEV, EXPERTS, TOP, CAP, 2))(routes_fake_keys, routes_fake_turns).reshape((TOKENS, TOP))
    gates_fake = jnp.clip(jnp.exp(math.log(1.0) - 1.609438 * jax.random.uniform(seeds[7], (TOKENS, TOP), jnp.float32) ** block_scale(seeds[7], (TOKENS, TOP), ((0, 16),), -0.2, 0.2)), 0.2, 1.0)
    cotangent = scatter_about(seeds[8], (TOKENS, D), 1.0, 6.0, ((0, 16), (1, 16)))
    up_fake = scatter_about(seeds[9], (EXPERTS, D, FF), D ** -0.5, 0.125, ((0, 8), (2, 16)))
    down_fake = scatter_about(seeds[10], (EXPERTS, FF, D), FF ** -0.5, 0.0625, ((0, 8), (1, 16)))
    return dict(x_real=x_real, routes_real=routes_real, gates_real=gates_real, up_real=up_real, down_real=down_real, x_fake=x_fake, routes_fake=routes_fake, gates_fake=gates_fake, cotangent=cotangent, up_fake=up_fake, down_fake=down_fake)


slope_const = 0.7978845608028654
cubic_coef = 0.044715


def gelu_tanh(value):
    return 0.5 * value * (1.0 + jnp.tanh(slope_const * (value + cubic_coef * value * value * value)))


def gelu_slope(value):
    inner = jnp.tanh(slope_const * (value + cubic_coef * value * value * value))
    return 0.5 * (1.0 + inner) + 0.5 * value * (1.0 - inner * inner) * slope_const * (1.0 + 3.0 * cubic_coef * value * value)


def slot_index(routes):
    blocks = routes.reshape(-1, TOK_DEV, TOP)
    labels = jnp.arange(EXPERTS, dtype=jnp.int32)
    hits = (blocks[:, :, :, None] == labels[None, None, None, :]).astype(jnp.int32)
    per_token = jnp.sum(hits, axis=2)
    before = jnp.cumsum(per_token, axis=1) - per_token
    return jnp.sum(hits * before[:, :, None, :], axis=3).reshape(-1, TOP).astype(jnp.int32)


def block_index():
    column = (jnp.arange(TOKENS, dtype=jnp.int32) // TOK_DEV)[:, None]
    return jnp.broadcast_to(column, (TOKENS, TOP)).astype(jnp.int32)


def to_buffer(rows, routes, slots, block):
    count = TOKENS // TOK_DEV
    width = rows.shape[-1]
    buffer = jnp.zeros((EXPERTS, count, CAP, width), rows.dtype)
    return buffer.at[routes, block, slots].set(rows).reshape(EXPERTS, count * CAP, width)


def reference(x_real, routes_real, gates_real, up_real, down_real, x_fake, routes_fake, gates_fake, cotangent, up_fake, down_fake):
    count = TOKENS // TOK_DEV
    block = block_index()
    slots_real = slot_index(routes_real)
    spread_x = jnp.broadcast_to(x_real[:, None, :], (TOKENS, TOP, D))
    buffer_real = to_buffer(spread_x, routes_real, slots_real, block)

    def run_real(item):
        rows, w_up, w_down = item
        hidden = gelu_tanh(jnp.dot(rows, w_up, preferred_element_type=jnp.float32)).astype(jnp.bfloat16)
        return jnp.dot(hidden, w_down, preferred_element_type=jnp.float32).astype(jnp.bfloat16)

    outputs = lax.map(run_real, (buffer_real, up_real, down_real))
    picked = outputs.reshape(EXPERTS, count, CAP, D)[routes_real, block, slots_real]
    real_out = jnp.sum(gates_real[:, :, None] * picked.astype(jnp.float32), axis=1).astype(jnp.bfloat16)

    slots_fake = slot_index(routes_fake)
    scaled = (gates_fake[:, :, None] * cotangent[:, None, :].astype(jnp.float32)).astype(jnp.bfloat16)
    spread_f = jnp.broadcast_to(x_fake[:, None, :], (TOKENS, TOP, D))
    buffer_x = to_buffer(spread_f, routes_fake, slots_fake, block)
    buffer_d = to_buffer(scaled, routes_fake, slots_fake, block)

    def run_fake(item):
        rows_x, rows_d, w_up, w_down = item
        pre = jnp.dot(rows_x, w_up, preferred_element_type=jnp.float32)
        act = gelu_tanh(pre).astype(jnp.bfloat16)
        back = lax.dot_general(rows_d, w_down, (((1,), (1,)), ((), ())), preferred_element_type=jnp.float32)
        dpre = (back * gelu_slope(pre)).astype(jnp.bfloat16)
        grad_in = lax.dot_general(rows_x, dpre, (((0,), (0,)), ((), ())), preferred_element_type=jnp.float32)
        grad_out = lax.dot_general(act, rows_d, (((0,), (0,)), ((), ())), preferred_element_type=jnp.float32)
        return grad_in.astype(jnp.bfloat16), grad_out.astype(jnp.bfloat16)

    grad_up, grad_down = lax.map(run_fake, (buffer_x, buffer_d, up_fake, down_fake))
    return (real_out, grad_up, grad_down)
```

```python
import jax
import jax.numpy as jnp
from jax import lax
from jax.sharding import Mesh
from jax.sharding import PartitionSpec as P

TENSOR = ("tensor_0", "tensor_1")


slope_const = 0.7978845608028654
cubic_coef = 0.044715


def in_order(pieces, dim):
    pieces = jnp.moveaxis(pieces, 0, dim)
    dims = pieces.shape
    return pieces.reshape(*dims[:dim], dims[dim] * dims[dim + 1], *dims[dim + 2 :])


def sent_to_all(x, axis):
    copies = jnp.broadcast_to(x, (lax.axis_size(axis), *x.shape))
    return lax.all_to_all(copies, axis, split_axis=0, concat_axis=0, tiled=True)


def gather_directly(x, axis, dim):
    return in_order(sent_to_all(x, axis), dim)


def reduced_to_own(pieces, axes, turns):
    dims = [lax.axis_size(a) for a in axes]
    pieces = pieces.reshape(*dims, *pieces.shape[1:])
    pieces = pieces.transpose(*turns, *range(len(axes), pieces.ndim))
    pieces = pieces.reshape(-1, *pieces.shape[len(axes) :])
    for k in turns:
        pieces = lax.psum_scatter(pieces, axes[k], scatter_dimension=0, tiled=True)
    return pieces[0]


def in_blocks(x, dim, length):
    dims = x.shape
    pieces = x.reshape(*dims[:dim], length, dims[dim] // length, *dims[dim + 1 :])
    return jnp.moveaxis(pieces, dim, 0)


def sum_by_axis(x, axes, turns, dim):
    length = lax.axis_size(axes)
    return reduced_to_own(in_blocks(x, dim, length), axes, turns)


def sent_together(arrays, axis, dim, along):
    ends, at = ([], 0)
    for a in arrays[:-1]:
        at += a.shape[along]
        ends.append(at)
    both = jnp.concatenate(arrays, axis=along)
    return tuple(jnp.split(lax.all_gather(both, axis, axis=dim, tiled=True), ends, axis=along))


def in_one_piece(arrays, axis, split_dim, concat_dim, along):
    ends, at = ([], 0)
    for a in arrays[:-1]:
        at += a.shape[along]
        ends.append(at)
    both = jnp.concatenate(arrays, axis=along)
    return tuple(
        jnp.split(
            lax.all_to_all(both, axis, split_axis=split_dim, concat_axis=concat_dim, tiled=True),
            ends,
            axis=along,
        )
    )


def partner(value, axis, stride):
    mask = 2**stride
    pairs = [(source, source ^ mask) for source in range(lax.axis_size(axis))]
    return lax.ppermute(value, axis, pairs)


def gelu_tanh(value):
    return (
        0.5 * value * (1.0 + jnp.tanh(slope_const * (value + cubic_coef * value * value * value)))
    )


def gelu_slope(value):
    inner = jnp.tanh(slope_const * (value + cubic_coef * value * value * value))
    return 0.5 * (1.0 + inner) + 0.5 * value * (1.0 - inner * inner) * slope_const * (
        1.0 + 3.0 * cubic_coef * value * value
    )


def slot_index(routes, experts, capacity):
    labels = jnp.arange(experts, dtype=jnp.int32)
    hits = (routes[:, :, None] == labels[None, None, :]).astype(jnp.int32)
    per_token = jnp.sum(hits, axis=1)
    before = jnp.cumsum(per_token, axis=0) - per_token
    slots = jnp.sum(hits * before[:, None, :], axis=2)
    return routes * capacity + slots


def spread_matrix(position, total):
    columns = jnp.arange(total, dtype=jnp.int32)
    match = (position[:, :, None] == columns[None, None, :]).astype(jnp.float32)
    return jnp.sum(match, axis=1).astype(jnp.bfloat16)


def pick_matrix(position, total):
    columns = jnp.arange(total, dtype=jnp.int32)
    flat = position.reshape(-1)
    return (flat[:, None] == columns[None, :]).astype(jnp.bfloat16)


def to_slots(matrix, rows):
    return lax.dot_general(
        matrix, rows, (((0,), (0,)), ((), ())), preferred_element_type=jnp.float32
    )


def over_rows(left, right):
    return lax.dot_general(
        left, right, (((0,), (0,)), ((), ())), preferred_element_type=jnp.float32
    )


def scale_rows(gates, rows):
    scaled = gates[:, :, None] * rows[:, None, :].astype(jnp.float32)
    return scaled.astype(jnp.bfloat16).reshape(-1, rows.shape[1])


def on_device(
    x_real,
    routes_real,
    gates_real,
    up_real,
    down_real,
    x_fake,
    routes_fake,
    gates_fake,
    cotangent,
    up_fake,
    down_fake,
):
    experts = lax.axis_size("expert")
    tokens = x_real.shape[0]
    top = routes_real.shape[1]
    capacity = tokens // 2
    total = experts * capacity
    w_up = up_real[0]
    w_down = down_real[0]
    wf_up = up_fake[0]
    wf_down = down_fake[0]
    real_pos = slot_index(routes_real, experts, capacity)
    real_pick = spread_matrix(real_pos, total)
    whole = lax.all_gather(x_real, TENSOR, axis=1, tiled=True)

    fake_pos = slot_index(routes_fake, experts, capacity)
    fake_pick = spread_matrix(fake_pos, total)
    fake_flat = pick_matrix(fake_pos, total)
    part = x_fake.shape[1]
    sent_x = to_slots(fake_pick, x_fake).astype(jnp.bfloat16).reshape(experts, capacity, part)
    sent_d = (
        to_slots(fake_flat, scale_rows(gates_fake, cotangent))
        .astype(jnp.bfloat16)
        .reshape(experts, capacity, part)
    )
    got_x, got_d = in_one_piece((sent_x, sent_d), "expert", 0, 0, 1)
    both = jnp.concatenate((got_x.reshape(total, part), got_d.reshape(total, part)), axis=0)
    whole, both = lax.optimization_barrier((whole, both))
    both = lax.all_gather(both, TENSOR, axis=1, tiled=True)
    rows_x, rows_d = both[:total], both[total:]

    width = whole.shape[1]
    sent = to_slots(real_pick, whole).astype(jnp.bfloat16).reshape(experts, capacity, width)
    arrived = lax.all_to_all(sent, "expert", split_axis=0, concat_axis=0, tiled=True)
    rows = arrived.reshape(total, width)
    pre_real = jnp.dot(rows, w_up, preferred_element_type=jnp.float32)
    hidden = gelu_tanh(pre_real).astype(jnp.bfloat16)
    partial_out = jnp.dot(hidden, w_down, preferred_element_type=jnp.float32).astype(jnp.bfloat16)
    returned = lax.all_to_all(
        partial_out.reshape(experts, capacity, width),
        "expert",
        split_axis=0,
        concat_axis=0,
        tiled=True,
    ).reshape(total, width)
    columns = jnp.arange(total, dtype=jnp.int32)
    match = (real_pos[:, :, None] == columns[None, None, :]).astype(jnp.float32)
    weights = jnp.sum(match * gates_real[:, :, None], axis=1)
    high = weights.astype(jnp.bfloat16)
    low = (weights - high.astype(jnp.float32)).astype(jnp.bfloat16)
    combined = jnp.dot(high, returned, preferred_element_type=jnp.float32) + jnp.dot(
        low, returned, preferred_element_type=jnp.float32
    )
    real_out = sum_by_axis(combined, TENSOR, (1, 0), 1).astype(jnp.bfloat16)

    pre_fake = jnp.dot(rows_x, wf_up, preferred_element_type=jnp.float32)
    act = gelu_tanh(pre_fake).astype(jnp.bfloat16)
    back_act = lax.dot_general(
        rows_d, wf_down, (((1,), (1,)), ((), ())), preferred_element_type=jnp.float32
    )
    dpre = (back_act * gelu_slope(pre_fake)).astype(jnp.bfloat16)
    mine = lax.axis_index("dp")
    half = rows_x.shape[1] // 2
    own_x = lax.dynamic_slice_in_dim(rows_x, mine * half, half, 1)
    other_x = lax.dynamic_slice_in_dim(rows_x, (1 - mine) * half, half, 1)
    own_d = lax.dynamic_slice_in_dim(rows_d, mine * half, half, 1)
    other_d = lax.dynamic_slice_in_dim(rows_d, (1 - mine) * half, half, 1)
    peer_x, peer_d, peer_act, peer_dpre = partner((other_x, other_d, act, dpre), "dp", 0)
    grad_in = over_rows(own_x, dpre) + over_rows(peer_x, peer_dpre)
    grad_out = over_rows(act, own_d) + over_rows(peer_act, peer_d)
    return (real_out, grad_in.astype(jnp.bfloat16)[None], grad_out.astype(jnp.bfloat16)[None])


def solution(mesh):
    split = Mesh(
        mesh.devices.reshape(mesh.shape["expert"], 2, 8, mesh.shape["dp"]),
        ("expert", "tensor_0", "tensor_1", "dp"),
    )
    placed = (
        P(("expert", "dp"), TENSOR),
        P(("expert", "dp"), None),
        P(("expert", "dp"), None),
        P("expert", None, TENSOR),
        P("expert", TENSOR, None),
        P(("expert", "dp"), TENSOR),
        P(("expert", "dp"), None),
        P(("expert", "dp"), None),
        P(("expert", "dp"), TENSOR),
        P("expert", None, TENSOR),
        P("expert", TENSOR, None),
    )
    return jax.shard_map(
        on_device,
        mesh=split,
        in_specs=placed,
        out_specs=(
            P(("expert", "dp"), TENSOR),
            P("expert", "dp", TENSOR),
            P("expert", TENSOR, "dp"),
        ),
        check_vma=False,
    )
```

```python
import functools

import jax
import jax.numpy as jnp
from jax import lax
from jax.experimental import pallas as pl
from jax.experimental.pallas import tpu as pltpu
from jax.sharding import PartitionSpec as P

MESH = pl.DeviceIdType.MESH
BF = jnp.bfloat16
F32 = jnp.float32

slope_const = 0.7978845608028654
cubic_coef = 0.044715


def gelu_tanh(value):
    return (
        0.5 * value * (1.0 + jnp.tanh(slope_const * (value + cubic_coef * value * value * value)))
    )


def gelu_both(value):
    square = value * value
    inner = jnp.tanh(slope_const * (value + cubic_coef * square * value))
    act = 0.5 * value * (1.0 + inner)
    slope = 0.5 * (1.0 + inner) + 0.5 * value * (1.0 - inner * inner) * slope_const * (
        1.0 + 3.0 * cubic_coef * square
    )
    return act, slope


def slot_index(routes, experts, capacity):
    labels = jnp.arange(experts, dtype=jnp.int32)
    hits = (routes[:, :, None] == labels[None, None, :]).astype(jnp.int32)
    per_token = jnp.sum(hits, axis=1)
    before = jnp.cumsum(per_token, axis=0) - per_token
    slots = jnp.sum(hits * before[:, None, :], axis=2)
    return routes * capacity + slots


def spread_matrix(position, total):
    columns = jnp.arange(total, dtype=jnp.int32)
    match = (position[:, :, None] == columns[None, None, :]).astype(jnp.float32)
    return jnp.sum(match, axis=1).astype(BF)


def pick_matrix(position, total):
    columns = jnp.arange(total, dtype=jnp.int32)
    flat = position.reshape(-1)
    return (flat[:, None] == columns[None, :]).astype(BF)


def over_rows(left, right):
    return lax.dot_general(left, right, (((0,), (0,)), ((), ())), preferred_element_type=F32)


def scale_rows(gates, rows):
    scaled = gates[:, :, None] * rows[:, None, :].astype(F32)
    return scaled.astype(BF).reshape(-1, rows.shape[1])


def kernel(
    sizes,
    xr_ref,
    spread_ref,
    high_ref,
    low_ref,
    sx_ref,
    sd_ref,
    wru_hbm,
    wrd_hbm,
    wfu_hbm,
    wfd_hbm,
    out_ref,
    gu_ref,
    gd_ref,
    wru,
    wrd,
    wfu,
    wfd,
    xt,
    sent,
    rows,
    po,
    ret,
    xf,
    df,
    px,
    pd,
    act,
    dpre,
    pact,
    pdpre,
    slope,
    hidden,
    cs,
    rs,
    w_sem,
    loc_sem,
    xt_send,
    xt_yh,
    xt_recv,
    fd_send,
    fd_recv,
    f_send,
    f_yh,
    f_recv,
    rd_send,
    rd_recv,
    rt_send,
    rt_recv,
    rs_send,
    rs_recv,
    dp_send,
    dp_recv,
):
    ne, nz, cap = sizes
    e = lax.axis_index("expert")
    t = lax.axis_index("tensor")
    dp = lax.axis_index("dp")
    yh = t // nz
    z = t % nz
    oy = 1 - yh
    wide = nz * 128
    total = ne * cap

    def near(step):
        return (z + step + nz) % nz

    def cols(zz, sub):
        y = yh if sub == 0 else oy
        return pl.ds(pl.multiple_of(y * wide + zz * 128, 128), 128)

    def block(expert):
        return pl.ds(pl.multiple_of(expert * cap, cap), cap)

    def remote(src, dst, send, recv, where):
        pltpu.make_async_remote_copy(
            src_ref=src, dst_ref=dst, send_sem=send, recv_sem=recv, device_id=where, device_id_type=MESH
        ).start()

    def local(src, dst, sem):
        pltpu.make_async_copy(src, dst, sem).start()

    def landed(ref, sem):
        pltpu.make_async_copy(ref, ref, sem).wait()

    here = (e, t, dp)
    other = (e, oy * nz + z, dp)
    mate = (e, t, 1 - dp)
    sides = ((e, yh * nz + near(1), dp), (e, yh * nz + near(-1), dp))

    for i, (src, dst) in enumerate(((wru_hbm, wru), (wrd_hbm, wrd), (wfu_hbm, wfu), (wfd_hbm, wfd))):
        local(src, dst, w_sem.at[i])
    local(xr_ref, xt.at[:, cols(z, 0)], loc_sem)

    barrier = pltpu.get_barrier_semaphore()

    def greet_expert(k, _):
        pl.semaphore_signal(
            barrier, inc=1, device_id=((e + k) % ne, t, dp), device_id_type=MESH
        )
        return 0

    def greet_tensor(k, _):
        pl.semaphore_signal(
            barrier, inc=1, device_id=(e, (t + k) % (2 * nz), dp), device_id_type=MESH
        )
        return 0

    lax.fori_loop(1, ne, greet_expert, 0)
    lax.fori_loop(1, 2 * nz, greet_tensor, 0)
    pl.semaphore_signal(barrier, inc=1, device_id=mate, device_id_type=MESH)
    pl.semaphore_wait(barrier, ne + 2 * nz - 1)

    def ring_send(ref, zz, sub, way, dist, send, recv):
        remote(
            ref.at[:, cols(zz, sub)],
            ref.at[:, cols(zz, sub)],
            send,
            recv.at[way, dist - 1, sub],
            sides[way],
        )

    def ring_take(ref, dist, sub, send, recv):
        for way in (0, 1):
            if dist == nz // 2 and way != sub:
                continue
            zz = near(-dist if way == 0 else dist)
            landed(ref.at[:, cols(zz, sub)], recv.at[way, dist - 1, sub])
            if dist < nz // 2 - 1 or (dist == nz // 2 - 1 and way == sub):
                ring_send(ref, zz, sub, way, dist + 1, send, recv)

    local_x = pltpu.make_async_copy(xr_ref, xt.at[:, cols(z, 0)], loc_sem)
    local_x.wait()
    for way in (0, 1):
        ring_send(xt, z, 0, way, 1, xt_send, xt_recv)
    remote(xt.at[:, cols(z, 0)], xt.at[:, cols(z, 0)], xt_send, xt_yh, other)

    for i, (src, dst) in enumerate(((sx_ref, xf), (sd_ref, df))):

        def give(k, _, i=i, src=src, dst=dst):
            to = (e + k) % ne
            remote(
                src.at[block(to), :],
                dst.at[block(e), cols(z, 0)],
                fd_send.at[i],
                fd_recv.at[i],
                (to, t, dp),
            )
            return 0

        lax.fori_loop(1, ne, give, 0)
        local(src.at[block(e), :], dst.at[block(e), cols(z, 0)], fd_recv.at[i])

    def slot(zz, sub):
        sent[:, cols(zz, sub)] = jnp.dot(
            spread_ref[...], xt[:, cols(zz, sub)], preferred_element_type=F32
        ).astype(BF)

    def dispatch(zz, sub):
        def give(k, _):
            to = (e + k) % ne
            remote(
                sent.at[block(to), cols(zz, sub)],
                rows.at[block(e), cols(zz, sub)],
                rd_send,
                rd_recv,
                (to, t, dp),
            )
            return 0

        lax.fori_loop(1, ne, give, 0)

    def real_step(dist, sub):
        ring_take(xt, dist, sub, xt_send, xt_recv)
        if dist == nz // 2:
            slot(near(dist), sub)
            dispatch(near(dist), sub)
        else:
            slot(near(-dist), sub)
            slot(near(dist), sub)
            dispatch(near(-dist), sub)
            dispatch(near(dist), sub)

    slot(z, 0)
    landed(xt.at[:, cols(z, 1)], xt_yh)
    for way in (0, 1):
        ring_send(xt, z, 1, way, 1, xt_send, xt_recv)
    slot(z, 1)
    dispatch(z, 0)
    dispatch(z, 1)

    fakes = ((0, xf), (1, df))

    def fake_yh(i, ref):
        landed(ref.at[:, cols(z, 0)], fd_recv.at[i])
        remote(ref.at[:, cols(z, 0)], ref.at[:, cols(z, 0)], f_send.at[i], f_yh.at[i], other)

    def fake_own(i, ref, sub):
        if sub == 1:
            landed(ref.at[:, cols(z, 1)], f_yh.at[i])
        for way in (0, 1):
            ring_send(ref, z, sub, way, 1, f_send.at[i], f_recv.at[i])

    def fake_step(i, ref, dist, sub):
        ring_take(ref, dist, sub, f_send.at[i], f_recv.at[i])

    fake_yh(0, xf)
    fake_own(0, xf, 0)
    fake_yh(1, df)
    real_step(1, 0)
    real_step(1, 1)
    fake_own(0, xf, 1)
    real_step(2, 0)
    real_step(2, 1)
    fake_step(0, xf, 1, 0)
    real_step(3, 0)
    real_step(3, 1)
    real_step(4, 0)
    real_step(4, 1)
    local(sent.at[block(e), :], rows.at[block(e), :], rd_recv)
    fake_step(0, xf, 1, 1)
    fake_own(1, df, 0)
    fake_step(0, xf, 2, 0)
    fake_step(0, xf, 2, 1)
    fake_own(1, df, 1)
    fake_step(0, xf, 3, 0)
    fake_step(0, xf, 3, 1)

    chunk = 256
    for i, (src, dst) in enumerate(((wru_hbm, wru), (wrd_hbm, wrd), (wfu_hbm, wfu), (wfd_hbm, wfd))):
        pltpu.make_async_copy(src, dst, w_sem.at[i]).wait()
    landed(rows, rd_recv)

    def up(r, _):
        at = pl.ds(pl.multiple_of(r * chunk, chunk), chunk)
        pre = jnp.dot(rows[at, :], wru[...], preferred_element_type=F32)
        hidden[at, :] = gelu_tanh(pre).astype(BF)
        return 0

    lax.fori_loop(0, total // chunk, up, 0)

    def down(step):
        zz = near(1 + step)
        w = jnp.concatenate([wrd[:, cols(zz, 0)], wrd[:, cols(zz, 1)]], axis=1)

        def part(r, _):
            at = pl.ds(pl.multiple_of(r * chunk, chunk), chunk)
            got = jnp.dot(hidden[at, :], w, preferred_element_type=F32).astype(BF)
            po[at, cols(zz, 0)] = got[:, :128]
            po[at, cols(zz, 1)] = got[:, 128:]
            return 0

        lax.fori_loop(0, total // chunk, part, 0)

    def give_back(step):
        zz = near(1 + step)
        for sub in (0, 1):

            def give(k, _, sub=sub):
                to = (e + k) % ne
                remote(
                    po.at[block(to), cols(zz, sub)],
                    ret.at[block(e), cols(zz, sub)],
                    rt_send,
                    rt_recv.at[step, sub],
                    (to, t, dp),
                )
                return 0

            lax.fori_loop(1, ne, give, 0)
            local(po.at[block(e), cols(zz, sub)], ret.at[block(e), cols(zz, sub)], rt_recv.at[step, sub])

    down(0)
    for step in range(1, nz):
        down(step)
        give_back(step - 1)
    give_back(nz - 1)

    def combine(step):
        zz = near(1 + step)
        for sub in (0, 1):
            landed(ret.at[:, cols(zz, sub)], rt_recv.at[step, sub])
        got = jnp.concatenate([ret[:, cols(zz, 0)], ret[:, cols(zz, 1)]], axis=1)
        both = jnp.dot(high_ref[...], got, preferred_element_type=F32) + jnp.dot(
            low_ref[...], got, preferred_element_type=F32
        )
        both = both.astype(BF)
        cs[:, cols(zz, 0)] = both[:, :128]
        cs[:, cols(zz, 1)] = both[:, 128:]

    def reduce_send(step):
        zz = near(1 + step)
        for sub in (0, 1):
            if step == nz - 1 and sub == 0:
                local(cs.at[:, cols(zz, 0)], rs.at[t], rs_recv)
            else:
                y = yh if sub == 0 else oy
                remote(cs.at[:, cols(zz, sub)], rs.at[t], rs_send, rs_recv, (e, y * nz + zz, dp))

    mine = pl.ds(pl.multiple_of(dp * wide, 128), wide)
    theirs = pl.ds(pl.multiple_of((1 - dp) * wide, 128), wide)

    fake_step(0, xf, 4, 0)
    fake_step(0, xf, 4, 1)
    remote(xf.at[:, theirs], px, dp_send.at[0], dp_recv.at[0], mate)
    fake_step(1, df, 1, 0)

    def fake_up(r, _):
        at = pl.ds(pl.multiple_of(r * chunk, chunk), chunk)
        pre = jnp.dot(xf[at, :], wfu[...], preferred_element_type=F32)
        a, s = gelu_both(pre)
        act[at, :] = a.astype(BF)
        slope[at, :] = s
        return 0

    lax.fori_loop(0, total // chunk, fake_up, 0)
    fake_step(1, df, 1, 1)
    remote(act, pact, dp_send.at[1], dp_recv.at[1], mate)
    combine(0)
    fake_step(1, df, 2, 0)
    combine(1)
    reduce_send(0)
    fake_step(1, df, 2, 1)
    combine(2)
    reduce_send(1)
    fake_step(1, df, 3, 0)
    fake_step(1, df, 3, 1)
    combine(3)
    reduce_send(2)
    combine(4)
    reduce_send(3)
    combine(5)
    reduce_send(4)
    combine(6)
    reduce_send(5)
    combine(7)
    reduce_send(6)
    fake_step(1, df, 4, 0)
    fake_step(1, df, 4, 1)
    reduce_send(7)
    remote(df.at[:, theirs], pd, dp_send.at[2], dp_recv.at[2], mate)

    def fake_back(r, _):
        at = pl.ds(pl.multiple_of(r * chunk, chunk), chunk)
        back = lax.dot_general(
            df[at, :], wfd[...], (((1,), (1,)), ((), ())), preferred_element_type=F32
        )
        dpre[at, :] = (back * slope[at, :]).astype(BF)
        return 0

    lax.fori_loop(0, total // chunk, fake_back, 0)

    half = wide // 2

    for m in (0, 1):
        own = pl.ds(pl.multiple_of(dp * wide + m * half, 128), half)
        pl_m = pl.ds(m * half, half)
        if m == 0:
            landed(pact, dp_recv.at[1])
            landed(pd, dp_recv.at[2])
        gd_ref[:, pl_m] = (over_rows(act[...], df[:, own]) + over_rows(pact[...], pd[:, pl_m])).astype(BF)
        if m == 0:
            remote(dpre, pdpre, dp_send.at[3], dp_recv.at[3], mate)
    landed(px, dp_recv.at[0])
    landed(pdpre, dp_recv.at[3])
    for m in (0, 1):
        own = pl.ds(pl.multiple_of(dp * wide + m * half, 128), half)
        pl_m = pl.ds(m * half, half)
        gu_ref[pl_m, :] = (over_rows(xf[:, own], dpre[...]) + over_rows(px[:, pl_m], pdpre[...])).astype(BF)

    landed(rs, rs_recv)
    summed = rs[0].astype(F32)
    for i in range(1, 2 * nz):
        summed = summed + rs[i].astype(F32)
    out_ref[...] = summed.astype(BF)

    most = pl.ds(0, (2 * nz - 1) * 128)
    seven = pl.ds(0, (ne - 1) * cap)
    landed(xt.at[:, most], xt_send)
    for i, src in enumerate((sx_ref, sd_ref)):
        landed(src.at[seven, :], fd_send.at[i])
    for i, ref in fakes:
        landed(ref.at[:, most], f_send.at[i])
    landed(sent.at[seven, :], rd_send)
    landed(po.at[seven, :], rt_send)
    landed(cs.at[:, most], rs_send)
    landed(px, dp_send.at[0])
    landed(act, dp_send.at[1])
    landed(pd, dp_send.at[2])
    landed(dpre, dp_send.at[3])


def solution(mesh):
    ne, nt = mesh.shape["expert"], mesh.shape["tensor"]
    nz = nt // 2

    def on_device(
        x_real,
        routes_real,
        gates_real,
        up_real,
        down_real,
        x_fake,
        routes_fake,
        gates_fake,
        cotangent,
        up_fake,
        down_fake,
    ):
        tokens, part = x_real.shape
        cap = tokens // 2
        total = ne * cap
        width = up_real.shape[1]
        ff = up_real.shape[2]
        half = width // 2
        real_pos = slot_index(routes_real, ne, cap)
        slots = jnp.arange(total, dtype=jnp.int32)
        flipped = real_pos.T
        spread = (
            (flipped[0][None, :] == slots[:, None]) | (flipped[1][None, :] == slots[:, None])
        ).astype(BF)
        match = (real_pos[:, :, None] == slots[None, None, :]).astype(F32)
        weights = jnp.sum(match * gates_real[:, :, None], axis=1)
        high = weights.astype(BF)
        low = (weights - high.astype(F32)).astype(BF)
        fake_pos = slot_index(routes_fake, ne, cap)
        sx = over_rows(spread_matrix(fake_pos, total), x_fake).astype(BF)
        sd = over_rows(pick_matrix(fake_pos, total), scale_rows(gates_fake, cotangent)).astype(BF)
        vmem = pl.BlockSpec(memory_space=pltpu.VMEM)
        hbm = pl.BlockSpec(memory_space=pl.ANY)
        dma = pltpu.SemaphoreType.DMA
        real_out, grad_up, grad_down = pl.pallas_call(
            functools.partial(kernel, (ne, nz, cap)),
            out_shape=(
                jax.ShapeDtypeStruct((tokens, part), BF),
                jax.ShapeDtypeStruct((half, ff), BF),
                jax.ShapeDtypeStruct((ff, half), BF),
            ),
            in_specs=[vmem] * 6 + [hbm] * 4,
            out_specs=(vmem, vmem, vmem),
            scratch_shapes=[
                pltpu.VMEM((width, ff), BF),
                pltpu.VMEM((ff, width), BF),
                pltpu.VMEM((width, ff), BF),
                pltpu.VMEM((ff, width), BF),
                pltpu.VMEM((tokens, width), BF),
                pltpu.VMEM((total, width), BF),
                pltpu.VMEM((total, width), BF),
                pltpu.VMEM((total, width), BF),
                pltpu.VMEM((total, width), BF),
                pltpu.VMEM((total, width), BF),
                pltpu.VMEM((total, width), BF),
                pltpu.VMEM((total, half), BF),
                pltpu.VMEM((total, half), BF),
                pltpu.VMEM((total, ff), BF),
                pltpu.VMEM((total, ff), BF),
                pltpu.VMEM((total, ff), BF),
                pltpu.VMEM((total, ff), BF),
                pltpu.VMEM((total, ff), F32),
                pltpu.VMEM((total, ff), BF),
                pltpu.VMEM((tokens, width), BF),
                pltpu.VMEM((nt, tokens, part), BF),
                dma((4,)),
                dma,
                dma,
                dma,
                dma((2, nz // 2, 2)),
                dma((2,)),
                dma((2,)),
                dma((2,)),
                dma((2,)),
                dma((2, 2, nz // 2, 2)),
                dma,
                dma,
                dma,
                dma((nz, 2)),
                dma,
                dma,
                dma((4,)),
                dma((4,)),
            ],
            compiler_params=pltpu.CompilerParams(
                collective_id=0, has_side_effects=True, vmem_limit_bytes=62 * 1024 * 1024
            ),
        )(
            x_real,
            spread,
            high,
            low,
            sx,
            sd,
            up_real[0],
            down_real[0],
            up_fake[0],
            down_fake[0],
        )
        return real_out, grad_up[None], grad_down[None]

    placed = (
        P(("expert", "dp"), "tensor"),
        P(("expert", "dp"), None),
        P(("expert", "dp"), None),
        P("expert", None, "tensor"),
        P("expert", "tensor", None),
        P(("expert", "dp"), "tensor"),
        P(("expert", "dp"), None),
        P(("expert", "dp"), None),
        P(("expert", "dp"), "tensor"),
        P("expert", None, "tensor"),
        P("expert", "tensor", None),
    )
    return jax.shard_map(
        on_device,
        mesh=mesh,
        in_specs=placed,
        out_specs=(
            P(("expert", "dp"), "tensor"),
            P("expert", "dp", "tensor"),
            P("expert", "tensor", "dp"),
        ),
        check_vma=False,
    )
```

```python
import functools

import jax
import jax.numpy as jnp
from jax import lax
from jax.experimental import pallas as pl
from jax.experimental.pallas import tpu as pltpu
from jax.sharding import PartitionSpec as P

MESH = pl.DeviceIdType.MESH
BF = jnp.bfloat16
F32 = jnp.float32

slope_const = 0.7978845608028654
cubic_coef = 0.044715


def gelu_tanh(value):
    return (
        0.5 * value * (1.0 + jnp.tanh(slope_const * (value + cubic_coef * value * value * value)))
    )


def gelu_both(value):
    square = value * value
    inner = jnp.tanh(slope_const * (value + cubic_coef * square * value))
    act = 0.5 * value * (1.0 + inner)
    slope = 0.5 * (1.0 + inner) + 0.5 * value * (1.0 - inner * inner) * slope_const * (
        1.0 + 3.0 * cubic_coef * square
    )
    return act, slope


def over_rows(left, right):
    return lax.dot_general(left, right, (((0,), (0,)), ((), ())), preferred_element_type=F32)


def kernel(
    sizes,
    xr_ref,
    xk_ref,
    ct_ref,
    rr_ref,
    gr_ref,
    rf_ref,
    gf_ref,
    wru_hbm,
    wrd_hbm,
    wfu_hbm,
    wfd_hbm,
    out_ref,
    gu_ref,
    gd_ref,
    wru,
    wrd,
    wfu,
    wfd,
    spread,
    wt,
    high,
    low,
    sx,
    sd,
    xt,
    sent,
    rows,
    po,
    ret,
    xf,
    df,
    px,
    pd,
    act_t,
    pact_t,
    dpre,
    pdpre,
    slope,
    acc,
    hidden,
    cs,
    rs,
    mine_f,
    last,
    w_sem,
    loc_sem,
    xt_send,
    xt_yh,
    xt_recv,
    fd_send,
    fd_recv,
    f_send,
    f_recv,
    rd_send,
    rd_recv,
    rt_send,
    rt_recv,
    rs_send,
    rs_recv,
    la_send,
    la_recv,
    px_send,
    px_recv,
    pd_send,
    pd_recv,
    dp_send,
    dp_recv,
):
    ne, nz, cap = sizes
    e = lax.axis_index("expert")
    t = lax.axis_index("tensor")
    dp = lax.axis_index("dp")
    yh = t // nz
    z = t % nz
    oy = 1 - yh
    wide = nz * 128
    total = ne * cap

    def near(step):
        return (z + step + nz) % nz

    def cols(zz, sub):
        y = yh if sub == 0 else oy
        return pl.ds(pl.multiple_of(y * wide + zz * 128, 128), 128)

    def block(expert):
        return pl.ds(pl.multiple_of(expert * cap, cap), cap)

    def remote(src, dst, send, recv, where):
        pltpu.make_async_remote_copy(
            src_ref=src, dst_ref=dst, send_sem=send, recv_sem=recv, device_id=where, device_id_type=MESH
        ).start()

    def local(src, dst, sem):
        pltpu.make_async_copy(src, dst, sem).start()

    def landed(ref, sem):
        pltpu.make_async_copy(ref, ref, sem).wait()

    other = (e, oy * nz + z, dp)
    mate = (e, t, 1 - dp)
    sides = ((e, yh * nz + near(1), dp), (e, yh * nz + near(-1), dp))

    barrier = pltpu.get_barrier_semaphore()

    def greet_expert(k, _):
        for y in (yh, oy):
            pl.semaphore_signal(
                barrier, inc=1, device_id=((e + k) % ne, y * nz + z, dp), device_id_type=MESH
            )
        return 0

    def greet_tensor(k, _):
        pl.semaphore_signal(
            barrier, inc=1, device_id=(e, (t + k) % (2 * nz), dp), device_id_type=MESH
        )
        return 0

    lax.fori_loop(1, ne, greet_expert, 0)
    lax.fori_loop(1, 2 * nz, greet_tensor, 0)
    pl.semaphore_signal(barrier, inc=1, device_id=mate, device_id_type=MESH)
    local(xr_ref, xt.at[:, cols(z, 0)], loc_sem)
    for i, (src, dst) in enumerate(((wru_hbm, wru), (wrd_hbm, wrd), (wfu_hbm, wfu), (wfd_hbm, wfd))):
        local(src, dst, w_sem.at[i])

    tokens = xr_ref.shape[0]
    chunk = 256
    earlier = (
        lax.broadcasted_iota(jnp.int32, (tokens, tokens), 0)
        < lax.broadcasted_iota(jnp.int32, (tokens, tokens), 1)
    ).astype(F32).astype(BF)
    labels = lax.broadcasted_iota(jnp.int32, (2 * ne, tokens), 0)

    def places(routes):
        hits = [(labels == routes[k : k + 1, :]).astype(F32) for k in (0, 1)]
        before = jnp.dot(
            (hits[0] + hits[1]).astype(BF), earlier, preferred_element_type=F32
        )
        return [
            routes[k : k + 1, :] * cap
            + jnp.sum(hits[k] * before, axis=0, keepdims=True).astype(jnp.int32)
            for k in (0, 1)
        ]

    def matches(at, places_of):
        slots = at * chunk + lax.broadcasted_iota(jnp.int32, (chunk, tokens), 0)
        return [slots == p for p in places_of]

    def weigh(masks, gates):
        return jnp.where(masks[0], gates[0:1, :], 0.0) + jnp.where(masks[1], gates[1:2, :], 0.0)

    fake_places = places(rf_ref[...])

    def fake_slots(r, _):
        at = pl.ds(pl.multiple_of(r * chunk, chunk), chunk)
        masks = matches(r, fake_places)
        pick = (masks[0] | masks[1]).astype(F32).astype(BF)
        sx[at, :] = jnp.dot(pick, xk_ref[...], preferred_element_type=F32).astype(BF)
        gate = jnp.sum(weigh(masks, gf_ref[...]), axis=1, keepdims=True)
        sd[at, :] = (gate * jnp.dot(pick, ct_ref[...], preferred_element_type=F32)).astype(BF)
        return 0

    lax.fori_loop(0, total // chunk, fake_slots, 0)
    real_places = places(rr_ref[...])

    def real_slots(r, _):
        at = pl.ds(pl.multiple_of(r * chunk, chunk), chunk)
        masks = matches(r, real_places)
        spread[at, :] = (masks[0] | masks[1]).astype(F32).astype(BF)
        wt[at, :] = weigh(masks, gr_ref[...])
        return 0

    lax.fori_loop(0, total // chunk, real_slots, 0)
    pl.semaphore_wait(barrier, 2 * (ne - 1) + 2 * nz)

    def ring_send(ref, zz, sub, way, dist, send, recv):
        remote(
            ref.at[:, cols(zz, sub)],
            ref.at[:, cols(zz, sub)],
            send,
            recv.at[way, dist - 1, sub],
            sides[way],
        )

    def ring_take(ref, dist, sub, send, recv):
        for way in (0, 1):
            if dist == nz // 2 and way != sub:
                continue
            zz = near(-dist if way == 0 else dist)
            landed(ref.at[:, cols(zz, sub)], recv.at[way, dist - 1, sub])
            if dist < nz // 2 - 1 or (dist == nz // 2 - 1 and way == sub):
                ring_send(ref, zz, sub, way, dist + 1, send, recv)

    local_x = pltpu.make_async_copy(xr_ref, xt.at[:, cols(z, 0)], loc_sem)
    local_x.wait()
    for way in (0, 1):
        ring_send(xt, z, 0, way, 1, xt_send, xt_recv)
    remote(xt.at[:, cols(z, 0)], xt.at[:, cols(z, 0)], xt_send, xt_yh, other)

    def fake_give(i, src, dst):
        for far, y in ((0, yh), (1, oy)):

            def give(k, _, far=far, y=y):
                to = (e + k) % ne
                remote(
                    src.at[block(to), :],
                    dst.at[block(e), cols(z, 0)],
                    fd_send.at[i, far],
                    fd_recv.at[i, far],
                    (to, y * nz + z, dp),
                )
                return 0

            lax.fori_loop(1 - far, ne, give, 0)
        local(src.at[block(e), :], dst.at[block(e), cols(z, 0)], fd_recv.at[i, 0])

    fake_give(0, sx, xf)

    def slot(zz, sub):
        sent[:, cols(zz, sub)] = jnp.dot(
            spread[...], xt[:, cols(zz, sub)], preferred_element_type=F32
        ).astype(BF)

    def dispatch(zz, sub):
        def give(k, _):
            to = (e + k) % ne
            remote(
                sent.at[block(to), cols(zz, sub)],
                rows.at[block(e), cols(zz, sub)],
                rd_send,
                rd_recv,
                (to, t, dp),
            )
            return 0

        lax.fori_loop(1, ne, give, 0)

    def real_step(dist, sub):
        ring_take(xt, dist, sub, xt_send, xt_recv)
        if dist == nz // 2:
            slot(near(dist), sub)
            dispatch(near(dist), sub)
        else:
            slot(near(-dist), sub)
            slot(near(dist), sub)
            dispatch(near(-dist), sub)
            dispatch(near(dist), sub)

    slot(z, 0)
    landed(xt.at[:, cols(z, 1)], xt_yh)
    for way in (0, 1):
        ring_send(xt, z, 1, way, 1, xt_send, xt_recv)
    slot(z, 1)
    dispatch(z, 0)
    dispatch(z, 1)

    fakes = ((0, xf), (1, df))

    def fake_own(i, ref, sub):
        landed(ref.at[:, cols(z, sub)], fd_recv.at[i, sub])
        for way in (0, 1):
            ring_send(ref, z, sub, way, 1, f_send.at[i], f_recv.at[i])

    def fake_step(i, ref, dist, sub):
        ring_take(ref, dist, sub, f_send.at[i], f_recv.at[i])

    for dist in (1, 2, 3):
        real_step(dist, 0)
        real_step(dist, 1)
    fake_own(0, xf, 0)
    fake_own(0, xf, 1)
    real_step(4, 0)
    real_step(4, 1)
    local(sent.at[block(e), :], rows.at[block(e), :], rd_recv)
    fake_give(1, sd, df)
    weights = wt[...].T
    rounded = weights.astype(BF)
    high[...] = rounded
    low[...] = (weights - rounded.astype(F32)).astype(BF)
    fake_step(0, xf, 1, 0)
    fake_step(0, xf, 1, 1)
    fake_step(0, xf, 2, 0)
    fake_step(0, xf, 2, 1)
    fake_step(0, xf, 3, 0)
    fake_step(0, xf, 3, 1)

    for i, (src, dst) in enumerate(((wru_hbm, wru), (wrd_hbm, wrd), (wfu_hbm, wfu), (wfd_hbm, wfd))):
        pltpu.make_async_copy(src, dst, w_sem.at[i]).wait()
    landed(rows, rd_recv)

    def up(r, _):
        at = pl.ds(pl.multiple_of(r * chunk, chunk), chunk)
        pre = jnp.dot(rows[at, :], wru[...], preferred_element_type=F32)
        hidden[at, :] = gelu_tanh(pre).astype(BF)
        return 0

    lax.fori_loop(0, total // chunk, up, 0)

    turns = [nz // 2] + [way * d for d in range(nz // 2 - 1, 0, -1) for way in (-1, 1)] + [0]

    def down(step):
        zz = near(turns[step])
        w = jnp.concatenate([wrd[:, cols(zz, 0)], wrd[:, cols(zz, 1)]], axis=1)

        def part(r, _):
            at = pl.ds(pl.multiple_of(r * chunk, chunk), chunk)
            got = jnp.dot(hidden[at, :], w, preferred_element_type=F32).astype(BF)
            po[at, cols(zz, 0)] = got[:, :128]
            po[at, cols(zz, 1)] = got[:, 128:]
            return 0

        lax.fori_loop(0, total // chunk, part, 0)

    def give_back(step):
        zz = near(turns[step])
        for sub in (0, 1):

            def give(k, _, sub=sub):
                to = (e + k) % ne
                remote(
                    po.at[block(to), cols(zz, sub)],
                    ret.at[block(e), cols(zz, sub)],
                    rt_send,
                    rt_recv.at[step, sub],
                    (to, t, dp),
                )
                return 0

            lax.fori_loop(1, ne, give, 0)
            local(po.at[block(e), cols(zz, sub)], ret.at[block(e), cols(zz, sub)], rt_recv.at[step, sub])

    down(0)
    for step in range(1, nz):
        down(step)
        give_back(step - 1)
        if step == 2:
            fake_own(1, df, 0)
        if step == 5:
            fake_own(1, df, 1)
    give_back(nz - 1)

    def combine(step):
        turn = turns[step]
        dist = abs(turn)
        zz = near(turn)
        for sub in (0, 1):
            landed(ret.at[:, cols(zz, sub)], rt_recv.at[step, sub])
        got = jnp.concatenate([ret[:, cols(zz, 0)], ret[:, cols(zz, 1)]], axis=1)
        both = jnp.dot(high[...], got, preferred_element_type=F32) + jnp.dot(
            low[...], got, preferred_element_type=F32
        )
        left, right = pl.ds(0, 128), pl.ds(128, 128)
        if dist == nz // 2:
            cs[step] = both.astype(BF)
            for way, half in ((0, left), (1, right)):
                remote(
                    cs.at[step, :, half],
                    rs.at[way, dist - 1, :, half],
                    rs_send,
                    rs_recv.at[way, dist - 1],
                    sides[way],
                )
        elif dist > 0:
            way = 0 if turn > 0 else 1
            if dist == nz // 2 - 1:
                half = (left, right)[way]
                landed(rs.at[way, dist, :, half], rs_recv.at[way, dist])
                cs[step] = both.astype(BF)
                more = both[:, way * 128 : (way + 1) * 128] + rs[way, dist, :, half].astype(F32)
                cs[step, :, half] = more.astype(BF)
            else:
                landed(rs.at[way, dist], rs_recv.at[way, dist])
                cs[step] = (both + rs[way, dist].astype(F32)).astype(BF)
            remote(
                cs.at[step], rs.at[way, dist - 1], rs_send, rs_recv.at[way, dist - 1], sides[way]
            )
        else:
            for way in (0, 1):
                landed(rs.at[way, 0], rs_recv.at[way, 0])
            both = both + rs[0, 0].astype(F32) + rs[1, 0].astype(F32)
            mine_f[...] = both[:, :128]
            cs[step, :, right] = both[:, 128:].astype(BF)
            remote(cs.at[step, :, right], last, la_send, la_recv, other)

    def half_cols(zz, side):
        return pl.ds(pl.multiple_of(side * wide + zz * 128, 128), 128)

    def fake_up(r, _):
        at = pl.ds(pl.multiple_of(r * chunk, chunk), chunk)
        pre = jnp.dot(xf[at, :], wfu[...], preferred_element_type=F32)
        a, s = gelu_both(pre)
        act_t[:, at] = a.T.astype(BF)
        slope[at, :] = s
        return 0

    def fake_mate(dist):
        for n, zz in enumerate(pair_of(dist)):
            at = pl.ds(pl.multiple_of(zz * 128, 128), 128)
            remote(df.at[:, half_cols(zz, 1 - dp)], pd.at[:, at], pd_send, pd_recv.at[dist, n], mate)

    def pair_of(dist):
        return (near(dist),) if dist in (0, nz // 2) else (near(-dist), near(dist))

    def back_part(dist):
        for zz in pair_of(dist):
            w = jnp.concatenate([wfd[:, cols(zz, 0)], wfd[:, cols(zz, 1)]], axis=1)

            def part(r, _, zz=zz, w=w):
                at = pl.ds(pl.multiple_of(r * chunk, chunk), chunk)
                rows_d = jnp.concatenate([df[at, cols(zz, 0)], df[at, cols(zz, 1)]], axis=1)
                back = lax.dot_general(
                    rows_d, w, (((1,), (1,)), ((), ())), preferred_element_type=F32
                )
                if dist == 0:
                    acc[at, :] = back
                elif dist == nz // 2:
                    dpre[at, :] = ((acc[at, :] + back) * slope[at, :]).astype(BF)
                else:
                    acc[at, :] += back
                return 0

            lax.fori_loop(0, total // chunk, part, 0)

    def grad_down_part(dist):
        zs = pair_of(dist)
        ats = [pl.ds(pl.multiple_of(zz * 128, 128), 128) for zz in zs]
        for n, at in enumerate(ats):
            landed(pd.at[:, at], pd_recv.at[dist, n])
        own = [df[:, half_cols(zz, dp)] for zz in zs]
        got = [pd[:, at] for at in ats]
        if len(zs) == 2:
            own, got = [jnp.concatenate(own, axis=1)], [jnp.concatenate(got, axis=1)]
        grad = jnp.dot(act_t[...], own[0], preferred_element_type=F32) + jnp.dot(
            pact_t[...], got[0], preferred_element_type=F32
        )
        grad = grad.astype(BF)
        for n, at in enumerate(ats):
            gd_ref[:, at] = grad[:, n * 128 : (n + 1) * 128]

    theirs = pl.ds(pl.multiple_of((1 - dp) * wide, 128), wide)

    fake_step(0, xf, 4, 0)
    fake_step(0, xf, 4, 1)
    remote(xf.at[:, theirs], px, px_send, px_recv, mate)
    lax.fori_loop(0, total // chunk, fake_up, 0)
    fake_step(1, df, 1, 0)
    combine(0)
    remote(act_t, pact_t, dp_send.at[0], dp_recv.at[0], mate)
    fake_mate(0)
    fake_step(1, df, 1, 1)
    fake_mate(1)
    combine(1)
    back_part(0)
    back_part(1)
    combine(2)
    fake_step(1, df, 2, 0)
    landed(pact_t, dp_recv.at[0])
    grad_down_part(0)
    grad_down_part(1)
    combine(3)
    fake_step(1, df, 2, 1)
    fake_mate(2)
    combine(4)
    back_part(2)
    fake_step(1, df, 3, 0)
    combine(5)
    grad_down_part(2)
    fake_step(1, df, 3, 1)
    fake_mate(3)
    combine(6)
    back_part(3)
    grad_down_part(3)
    combine(7)
    fake_step(1, df, 4, 0)
    fake_step(1, df, 4, 1)
    fake_mate(4)
    back_part(4)
    remote(dpre, pdpre, dp_send.at[1], dp_recv.at[1], mate)
    grad_down_part(4)
    landed(px, px_recv)
    half = wide // 2
    for m in (0, 1):
        own = pl.ds(pl.multiple_of(dp * wide + m * half, 128), half)
        acc[m * half : (m + 1) * half, :] = over_rows(xf[:, own], dpre[...])
    landed(last, la_recv)
    out_ref[...] = (mine_f[...] + last[...].astype(F32)).astype(BF)
    landed(pdpre, dp_recv.at[1])
    for m in (0, 1):
        at = slice(m * half, (m + 1) * half)
        gu_ref[at, :] = (acc[at, :] + over_rows(px[:, at], pdpre[...])).astype(BF)

    most = pl.ds(0, (2 * nz - 1) * 128)
    seven = pl.ds(0, (ne - 1) * cap)
    landed(xt.at[:, most], xt_send)
    for i, src in enumerate((sx, sd)):
        landed(src.at[seven, :], fd_send.at[i, 0])
        landed(src, fd_send.at[i, 1])
    for i, ref in fakes:
        landed(ref.at[:, pl.ds(0, (2 * nz - 2) * 128)], f_send.at[i])
    landed(sent.at[seven, :], rd_send)
    landed(po.at[seven, :], rt_send)
    landed(cs.at[pl.ds(0, nz - 1)], rs_send)
    landed(last, la_send)
    landed(px, px_send)
    landed(pd, pd_send)
    landed(act_t, dp_send.at[0])
    landed(dpre, dp_send.at[1])


def solution(mesh):
    ne, nt = mesh.shape["expert"], mesh.shape["tensor"]
    nz = nt // 2

    def on_device(
        x_real,
        routes_real,
        gates_real,
        up_real,
        down_real,
        x_fake,
        routes_fake,
        gates_fake,
        cotangent,
        up_fake,
        down_fake,
    ):
        tokens, part = x_real.shape
        cap = tokens // 2
        total = ne * cap
        width = up_real.shape[1]
        ff = up_real.shape[2]
        half = width // 2
        vmem = pl.BlockSpec(memory_space=pltpu.VMEM)
        hbm = pl.BlockSpec(memory_space=pl.ANY)
        dma = pltpu.SemaphoreType.DMA
        real_out, grad_up, grad_down = pl.pallas_call(
            functools.partial(kernel, (ne, nz, cap)),
            out_shape=(
                jax.ShapeDtypeStruct((tokens, part), BF),
                jax.ShapeDtypeStruct((half, ff), BF),
                jax.ShapeDtypeStruct((ff, half), BF),
            ),
            in_specs=[vmem] * 7 + [hbm] * 4,
            out_specs=(vmem, vmem, vmem),
            scratch_shapes=[
                pltpu.VMEM((width, ff), BF),
                pltpu.VMEM((ff, width), BF),
                pltpu.VMEM((width, ff), BF),
                pltpu.VMEM((ff, width), BF),
                pltpu.VMEM((total, tokens), BF),
                pltpu.VMEM((total, tokens), F32),
                pltpu.VMEM((tokens, total), BF),
                pltpu.VMEM((tokens, total), BF),
                pltpu.VMEM((total, part), BF),
                pltpu.VMEM((total, part), BF),
                pltpu.VMEM((tokens, width), BF),
                pltpu.VMEM((total, width), BF),
                pltpu.VMEM((total, width), BF),
                pltpu.VMEM((total, width), BF),
                pltpu.VMEM((total, width), BF),
                pltpu.VMEM((total, width), BF),
                pltpu.VMEM((total, width), BF),
                pltpu.VMEM((total, half), BF),
                pltpu.VMEM((total, half), BF),
                pltpu.VMEM((ff, total), BF),
                pltpu.VMEM((ff, total), BF),
                pltpu.VMEM((total, ff), BF),
                pltpu.VMEM((total, ff), BF),
                pltpu.VMEM((total, ff), F32),
                pltpu.VMEM((total, ff), F32),
                pltpu.VMEM((total, ff), BF),
                pltpu.VMEM((nz, tokens, 2 * part), BF),
                pltpu.VMEM((2, nz // 2, tokens, 2 * part), BF),
                pltpu.VMEM((tokens, part), F32),
                pltpu.VMEM((tokens, part), BF),
                dma((4,)),
                dma,
                dma,
                dma,
                dma((2, nz // 2, 2)),
                dma((2, 2)),
                dma((2, 2)),
                dma((2,)),
                dma((2, 2, nz // 2, 2)),
                dma,
                dma,
                dma,
                dma((nz, 2)),
                dma,
                dma((2, nz // 2)),
                dma,
                dma,
                dma,
                dma,
                dma,
                dma((nz // 2 + 1, 2)),
                dma((2,)),
                dma((2,)),
            ],
            compiler_params=pltpu.CompilerParams(
                collective_id=0, has_side_effects=True, vmem_limit_bytes=62 * 1024 * 1024
            ),
        )(
            x_real,
            x_fake,
            cotangent,
            routes_real.T,
            gates_real.T,
            routes_fake.T,
            gates_fake.T,
            up_real[0],
            down_real[0],
            up_fake[0],
            down_fake[0],
        )
        return real_out, grad_up[None], grad_down[None]

    placed = (
        P(("expert", "dp"), "tensor"),
        P(("expert", "dp"), None),
        P(("expert", "dp"), None),
        P("expert", None, "tensor"),
        P("expert", "tensor", None),
        P(("expert", "dp"), "tensor"),
        P(("expert", "dp"), None),
        P(("expert", "dp"), None),
        P(("expert", "dp"), "tensor"),
        P("expert", None, "tensor"),
        P("expert", "tensor", None),
    )
    return jax.shard_map(
        on_device,
        mesh=mesh,
        in_specs=placed,
        out_specs=(
            P(("expert", "dp"), "tensor"),
            P("expert", "dp", "tensor"),
            P("expert", "tensor", "dp"),
        ),
        check_vma=False,
    )
```

```python
import functools

import jax
import jax.numpy as jnp
from jax import lax
from jax.experimental import pallas as pl
from jax.experimental.pallas import tpu as pltpu
from jax.sharding import PartitionSpec as P

MESH = pl.DeviceIdType.MESH
BF = jnp.bfloat16
F32 = jnp.float32

slope_const = 0.7978845608028654
cubic_coef = 0.044715


def gelu_tanh(value):
    return (
        0.5 * value * (1.0 + jnp.tanh(slope_const * (value + cubic_coef * value * value * value)))
    )


def gelu_both(value):
    square = value * value
    inner = jnp.tanh(slope_const * (value + cubic_coef * square * value))
    act = 0.5 * value * (1.0 + inner)
    slope = 0.5 * (1.0 + inner) + 0.5 * value * (1.0 - inner * inner) * slope_const * (
        1.0 + 3.0 * cubic_coef * square
    )
    return act, slope


def over_rows(left, right):
    return lax.dot_general(left, right, (((0,), (0,)), ((), ())), preferred_element_type=F32)


def kernel(
    sizes,
    xr_ref,
    xk_ref,
    ct_ref,
    rr_ref,
    gr_ref,
    rf_ref,
    gf_ref,
    wru_hbm,
    wrd_hbm,
    wfu_hbm,
    wfd_hbm,
    out_hbm,
    gu_hbm,
    gd_hbm,
    out_ref,
    gu_ref,
    gd_ref,
    xo_t,
    px_t,
    wru,
    wrd,
    wfu,
    wfd,
    spread,
    wt,
    high,
    low,
    sx,
    sd,
    xt,
    sent,
    rows,
    po,
    ret,
    xf,
    df,
    px,
    pd,
    act_t,
    pact_t,
    dpre,
    pdpre,
    slope,
    acc,
    hidden,
    cs,
    rs,
    mine_f,
    last,
    w_sem,
    o_sem,
    loc_sem,
    xt_send,
    xt_yh,
    xt_recv,
    fd_send,
    fd_recv,
    f_send,
    f_recv,
    rd_send,
    rd_recv,
    rh_recv,
    rt_send,
    rt_recv,
    rth_recv,
    rs_send,
    rs_recv,
    la_send,
    la_recv,
    px_send,
    px_recv,
    pd_send,
    pd_recv,
    dp_send,
    dp_recv,
):
    ne, nz, cap = sizes
    e = lax.axis_index("expert")
    t = lax.axis_index("tensor")
    dp = lax.axis_index("dp")
    yh = t // nz
    z = t % nz
    oy = 1 - yh
    wide = nz * 128
    total = ne * cap

    def near(step):
        return (z + step + nz) % nz

    def cols(zz, sub):
        y = yh if sub == 0 else oy
        return pl.ds(pl.multiple_of(y * wide + zz * 128, 128), 128)

    def block(expert):
        return pl.ds(pl.multiple_of(expert * cap, cap), cap)

    def remote(src, dst, send, recv, where):
        pltpu.make_async_remote_copy(
            src_ref=src, dst_ref=dst, send_sem=send, recv_sem=recv, device_id=where, device_id_type=MESH
        ).start()

    def local(src, dst, sem):
        pltpu.make_async_copy(src, dst, sem).start()

    def landed(ref, sem):
        pltpu.make_async_copy(ref, ref, sem).wait()

    other = (e, oy * nz + z, dp)
    mate = (e, t, 1 - dp)
    sides = ((e, yh * nz + near(1), dp), (e, yh * nz + near(-1), dp))

    barrier = pltpu.get_barrier_semaphore()

    def greet_expert(k, _):
        for y in (yh, oy):
            pl.semaphore_signal(
                barrier, inc=1, device_id=((e + k) % ne, y * nz + z, dp), device_id_type=MESH
            )
        return 0

    lax.fori_loop(1, ne, greet_expert, 0)
    for peer in (*sides, other):
        pl.semaphore_signal(barrier, inc=1, device_id=peer, device_id_type=MESH)
    pl.semaphore_signal(barrier, inc=1, device_id=mate, device_id_type=MESH)
    local(xr_ref, xt.at[:, cols(z, 0)], loc_sem)
    for i, (src, dst) in enumerate(((wru_hbm, wru), (wrd_hbm, wrd), (wfu_hbm, wfu), (wfd_hbm, wfd))):
        local(src, dst, w_sem.at[i])

    tokens = xr_ref.shape[0]
    chunk = 256
    earlier = (
        lax.broadcasted_iota(jnp.int32, (tokens, tokens), 0)
        < lax.broadcasted_iota(jnp.int32, (tokens, tokens), 1)
    ).astype(F32).astype(BF)
    labels = lax.broadcasted_iota(jnp.int32, (2 * ne, tokens), 0)

    def places(routes):
        hits = [(labels == routes[k : k + 1, :]).astype(F32) for k in (0, 1)]
        before = jnp.dot(
            (hits[0] + hits[1]).astype(BF), earlier, preferred_element_type=F32
        )
        return [
            routes[k : k + 1, :] * cap
            + jnp.sum(hits[k] * before, axis=0, keepdims=True).astype(jnp.int32)
            for k in (0, 1)
        ]

    def matches(at, places_of):
        slots = at * chunk + lax.broadcasted_iota(jnp.int32, (chunk, tokens), 0)
        return [slots == p for p in places_of]

    def weigh(masks, gates):
        return jnp.where(masks[0], gates[0:1, :], 0.0) + jnp.where(masks[1], gates[1:2, :], 0.0)

    fake_places = places(rf_ref[...])

    def fake_slots(r, _):
        at = pl.ds(pl.multiple_of(r * chunk, chunk), chunk)
        masks = matches(r, fake_places)
        pick = (masks[0] | masks[1]).astype(F32).astype(BF)
        sx[at, :] = jnp.dot(pick, xk_ref[...], preferred_element_type=F32).astype(BF)
        gate = jnp.sum(weigh(masks, gf_ref[...]), axis=1, keepdims=True)
        sd[at, :] = (gate * jnp.dot(pick, ct_ref[...], preferred_element_type=F32)).astype(BF)
        return 0

    lax.fori_loop(0, total // chunk, fake_slots, 0)
    real_places = places(rr_ref[...])

    def real_slots(r, _):
        at = pl.ds(pl.multiple_of(r * chunk, chunk), chunk)
        masks = matches(r, real_places)
        spread[at, :] = (masks[0] | masks[1]).astype(F32).astype(BF)
        wt[at, :] = weigh(masks, gr_ref[...])
        return 0

    lax.fori_loop(0, total // chunk, real_slots, 0)
    pl.semaphore_wait(barrier, 2 * (ne - 1) + 4)

    def ring_send(ref, zz, sub, way, dist, send, recv):
        remote(
            ref.at[:, cols(zz, sub)],
            ref.at[:, cols(zz, sub)],
            send,
            recv.at[way, dist - 1, sub],
            sides[way],
        )

    def ring_take(ref, dist, sub, send, recv):
        for way in (0, 1):
            if dist == nz // 2 and way != sub:
                continue
            zz = near(-dist if way == 0 else dist)
            landed(ref.at[:, cols(zz, sub)], recv.at[way, dist - 1, sub])
            if dist < nz // 2 - 1 or (dist == nz // 2 - 1 and way == sub):
                ring_send(ref, zz, sub, way, dist + 1, send, recv)

    local_x = pltpu.make_async_copy(xr_ref, xt.at[:, cols(z, 0)], loc_sem)
    local_x.wait()
    for way in (0, 1):
        ring_send(xt, z, 0, way, 1, xt_send, xt_recv)
    remote(xt.at[:, cols(z, 0)], xt.at[:, cols(z, 0)], xt_send, xt_yh, other)

    def fake_give(i, src, dst, far):
        y = oy if far else yh

        def give(k, _):
            to = (e + k) % ne
            remote(
                src.at[block(to), :],
                dst.at[block(e), cols(z, 0)],
                fd_send.at[i, far],
                fd_recv.at[i, far],
                (to, y * nz + z, dp),
            )
            return 0

        lax.fori_loop(1 - far, ne, give, 0)
        if not far:
            local(src.at[block(e), :], dst.at[block(e), cols(z, 0)], fd_recv.at[i, 0])

    fake_give(0, sx, xf, 0)

    def slot(zz, sub):
        sent[:, cols(zz, sub)] = jnp.dot(
            spread[...], xt[:, cols(zz, sub)], preferred_element_type=F32
        ).astype(BF)

    def pair_of(dist):
        return (near(dist),) if dist in (0, nz // 2) else (near(-dist), near(dist))

    def share(expert, part):
        if part is None:
            return block(expert)
        return pl.ds(pl.multiple_of(expert * cap + part * (cap // 2), cap // 2), cap // 2)

    def dispatch(dist, sub, part=None):
        for n, zz in enumerate(pair_of(dist)):
            recv = rd_recv.at[dist, n, sub] if part is None else rh_recv.at[dist, n, part]

            def give(k, _, zz=zz, recv=recv):
                to = (e + k) % ne
                remote(
                    sent.at[share(to, part), cols(zz, sub)],
                    rows.at[share(e, part), cols(zz, sub)],
                    rd_send,
                    recv,
                    (to, t, dp),
                )
                return 0

            lax.fori_loop(1, ne, give, 0)
            local(
                sent.at[share(e, part), cols(zz, sub)], rows.at[share(e, part), cols(zz, sub)], recv
            )

    late = (2, 3, 4)

    def real_step(dist, sub):
        ring_take(xt, dist, sub, xt_send, xt_recv)
        for zz in pair_of(dist):
            slot(zz, sub)
        dispatch(dist, sub, 0 if sub == 1 and dist in late else None)

    def up_part(dist, sub):
        where = [cols(zz, sub) for zz in pair_of(dist)]
        for n, zz in enumerate(pair_of(dist)):
            landed(rows.at[:, cols(zz, sub)], rd_recv.at[dist, n, sub])
        w = jnp.concatenate([wru[c, :] for c in where], axis=0)

        def part(r, _):
            at = pl.ds(pl.multiple_of(r * chunk, chunk), chunk)
            got = jnp.concatenate([rows[at, c] for c in where], axis=1)
            pre = jnp.dot(got, w, preferred_element_type=F32)
            if dist == 0 and sub == 0:
                acc[at, :] = pre
            else:
                acc[at, :] += pre
            return 0

        lax.fori_loop(0, total // chunk, part, 0)

    def halves(r, part):
        return [share(r * 4 + j, part) for j in range(4)]

    def up_half(part):
        where = [cols(zz, 1) for dist in late for zz in pair_of(dist)]
        for dist in late:
            for n, zz in enumerate(pair_of(dist)):
                half_bytes = rows.at[pl.ds(0, total // 2), cols(zz, 1)]
                landed(half_bytes, rh_recv.at[dist, n, part])
        w = jnp.concatenate([wru[c, :] for c in where], axis=0)

        def some(r, _):
            ats = halves(r, part)
            got = jnp.concatenate(
                [jnp.concatenate([rows[at, c] for c in where], axis=1) for at in ats], axis=0
            )
            pre = jnp.dot(got, w, preferred_element_type=F32)
            for j, at in enumerate(ats):
                own = acc[at, :] + pre[j * (cap // 2) : (j + 1) * (cap // 2), :]
                hidden[at, :] = gelu_tanh(own).astype(BF)
            return 0

        lax.fori_loop(0, ne // 4, some, 0)

    fakes = ((0, xf), (1, df))

    def fake_own(i, ref, sub):
        landed(ref.at[:, cols(z, sub)], fd_recv.at[i, sub])
        for way in (0, 1):
            ring_send(ref, z, sub, way, 1, f_send.at[i], f_recv.at[i])

    def fake_step(i, ref, dist, sub):
        ring_take(ref, dist, sub, f_send.at[i], f_recv.at[i])

    def fake_up(r, _):
        at = pl.ds(pl.multiple_of(r * chunk, chunk), chunk)
        pre = jnp.dot(xf[at, :], wfu[...], preferred_element_type=F32)
        a, s = gelu_both(pre)
        act_t[:, at] = a.T.astype(BF)
        slope[at, :] = s
        return 0

    theirs = pl.ds(pl.multiple_of((1 - dp) * wide, 128), wide)

    slot(z, 0)
    dispatch(0, 0)
    real_step(1, 0)
    fake_give(0, sx, xf, 1)
    real_step(2, 0)
    fake_own(0, xf, 0)
    real_step(3, 0)
    landed(xt.at[:, cols(z, 1)], xt_yh)
    for way in (0, 1):
        ring_send(xt, z, 1, way, 1, xt_send, xt_recv)
    slot(z, 1)
    dispatch(0, 1)
    real_step(1, 1)
    real_step(4, 0)
    fake_own(0, xf, 1)
    real_step(2, 1)
    fake_step(0, xf, 1, 0)
    fake_give(1, sd, df, 0)
    fake_give(1, sd, df, 1)
    real_step(3, 1)
    real_step(4, 1)
    for dist in late:
        dispatch(dist, 1, 1)
    weights = wt[...].T
    rounded = weights.astype(BF)
    high[...] = rounded
    low[...] = (weights - rounded.astype(F32)).astype(BF)
    for i, (src, dst) in enumerate(((wru_hbm, wru), (wrd_hbm, wrd), (wfu_hbm, wfu), (wfd_hbm, wfd))):
        pltpu.make_async_copy(src, dst, w_sem.at[i]).wait()
    up_part(0, 0)
    up_part(1, 0)
    fake_step(0, xf, 1, 1)
    up_part(2, 0)
    fake_step(0, xf, 2, 0)
    up_part(3, 0)
    up_part(4, 0)
    up_part(0, 1)
    fake_step(0, xf, 2, 1)
    up_part(1, 1)
    fake_step(0, xf, 3, 0)
    fake_own(1, df, 0)
    fake_own(1, df, 1)
    up_half(0)

    early = (0, 1)
    turns = [nz // 2] + [way * d for d in range(nz // 2 - 1, 0, -1) for way in (-1, 1)] + [0]

    def down(step, part=None):
        zz = near(turns[step])
        w = jnp.concatenate([wrd[:, cols(zz, 0)], wrd[:, cols(zz, 1)]], axis=1)

        def some(r, _):
            if part is None:
                ats = [pl.ds(pl.multiple_of(r * chunk, chunk), chunk)]
            else:
                ats = halves(r, part)
            got = [hidden[at, :] for at in ats]
            got = got[0] if part is None else jnp.concatenate(got, axis=0)
            got = jnp.dot(got, w, preferred_element_type=F32).astype(BF)
            size = chunk // len(ats)
            for j, at in enumerate(ats):
                po[at, cols(zz, 0)] = got[j * size : (j + 1) * size, :128]
                po[at, cols(zz, 1)] = got[j * size : (j + 1) * size, 128:]
            return 0

        lax.fori_loop(0, total // chunk if part is None else ne // 4, some, 0)

    def give_back(step, part=None):
        zz = near(turns[step])
        for sub in (0, 1):
            recv = rt_recv.at[step, sub] if part is None else rth_recv.at[step, sub, part]

            def give(k, _, sub=sub, recv=recv):
                to = (e + k) % ne
                remote(
                    po.at[share(to, part), cols(zz, sub)],
                    ret.at[share(e, part), cols(zz, sub)],
                    rt_send,
                    recv,
                    (to, t, dp),
                )
                return 0

            lax.fori_loop(1, ne, give, 0)
            local(
                po.at[share(e, part), cols(zz, sub)], ret.at[share(e, part), cols(zz, sub)], recv
            )

    for step in early:
        down(step, 0)
    for step in early:
        give_back(step, 0)
    fake_step(0, xf, 3, 1)
    up_half(1)
    for step in early:
        down(step, 1)
    for step in early:
        give_back(step, 1)
    down(len(early))
    for step in range(len(early) + 1, nz):
        down(step)
        give_back(step - 1)
        if step == nz // 2:
            fake_step(1, df, 1, 0)
    give_back(nz - 1)

    def combine(step):
        turn = turns[step]
        dist = abs(turn)
        zz = near(turn)
        for sub in (0, 1):
            if step in early:
                for part in (0, 1):
                    landed(ret.at[pl.ds(0, total // 2), cols(zz, sub)], rth_recv.at[step, sub, part])
            else:
                landed(ret.at[:, cols(zz, sub)], rt_recv.at[step, sub])
        got = jnp.concatenate([ret[:, cols(zz, 0)], ret[:, cols(zz, 1)]], axis=1)
        both = jnp.dot(high[...], got, preferred_element_type=F32) + jnp.dot(
            low[...], got, preferred_element_type=F32
        )
        left, right = pl.ds(0, 128), pl.ds(128, 128)
        if dist == nz // 2:
            cs[step] = both.astype(BF)
            for way, half in ((0, left), (1, right)):
                remote(
                    cs.at[step, :, half],
                    rs.at[way, dist - 1, :, half],
                    rs_send,
                    rs_recv.at[way, dist - 1],
                    sides[way],
                )
        elif dist > 0:
            way = 0 if turn > 0 else 1
            if dist == nz // 2 - 1:
                half = (left, right)[way]
                landed(rs.at[way, dist, :, half], rs_recv.at[way, dist])
                cs[step] = both.astype(BF)
                more = both[:, way * 128 : (way + 1) * 128] + rs[way, dist, :, half].astype(F32)
                cs[step, :, half] = more.astype(BF)
            else:
                landed(rs.at[way, dist], rs_recv.at[way, dist])
                cs[step] = (both + rs[way, dist].astype(F32)).astype(BF)
            remote(
                cs.at[step], rs.at[way, dist - 1], rs_send, rs_recv.at[way, dist - 1], sides[way]
            )
        else:
            for way in (0, 1):
                landed(rs.at[way, 0], rs_recv.at[way, 0])
            both = both + rs[0, 0].astype(F32) + rs[1, 0].astype(F32)
            mine_f[...] = both[:, :128]
            cs[step, :, right] = both[:, 128:].astype(BF)
            remote(cs.at[step, :, right], last, la_send, la_recv, other)

    def half_cols(zz, side):
        return pl.ds(pl.multiple_of(side * wide + zz * 128, 128), 128)

    def fake_mate(dist):
        for n, zz in enumerate(pair_of(dist)):
            at = pl.ds(pl.multiple_of(zz * 128, 128), 128)
            remote(df.at[:, half_cols(zz, 1 - dp)], pd.at[:, at], pd_send, pd_recv.at[dist, n], mate)

    def back_part(dist):
        for zz in pair_of(dist):
            w = jnp.concatenate([wfd[:, cols(zz, 0)], wfd[:, cols(zz, 1)]], axis=1)

            def part(r, _, zz=zz, w=w):
                at = pl.ds(pl.multiple_of(r * chunk, chunk), chunk)
                rows_d = jnp.concatenate([df[at, cols(zz, 0)], df[at, cols(zz, 1)]], axis=1)
                back = lax.dot_general(
                    rows_d, w, (((1,), (1,)), ((), ())), preferred_element_type=F32
                )
                if dist == 0:
                    acc[at, :] = back
                elif dist == nz // 2:
                    dpre[at, :] = ((acc[at, :] + back) * slope[at, :]).astype(BF)
                else:
                    acc[at, :] += back
                return 0

            lax.fori_loop(0, total // chunk, part, 0)

    def grad_down_part(dist):
        zs = pair_of(dist)
        ats = [pl.ds(pl.multiple_of(zz * 128, 128), 128) for zz in zs]
        for n, at in enumerate(ats):
            landed(pd.at[:, at], pd_recv.at[dist, n])
        own = [df[:, half_cols(zz, dp)] for zz in zs]
        got = [pd[:, at] for at in ats]
        if len(zs) == 2:
            own, got = [jnp.concatenate(own, axis=1)], [jnp.concatenate(got, axis=1)]
        grad = jnp.dot(act_t[...], own[0], preferred_element_type=F32) + jnp.dot(
            pact_t[...], got[0], preferred_element_type=F32
        )
        grad = grad.astype(BF)
        for n, at in enumerate(ats):
            gd_ref[:, at] = grad[:, n * 128 : (n + 1) * 128]

    fake_step(0, xf, 4, 0)
    fake_step(0, xf, 4, 1)
    remote(xf.at[:, theirs], px, px_send, px_recv, mate)
    lax.fori_loop(0, total // chunk, fake_up, 0)
    fake_step(1, df, 1, 1)
    remote(act_t, pact_t, dp_send.at[0], dp_recv.at[0], mate)
    fake_mate(0)
    fake_mate(1)
    combine(0)
    back_part(0)
    back_part(1)
    landed(pact_t, dp_recv.at[0])
    fake_step(1, df, 2, 0)
    grad_down_part(0)
    grad_down_part(1)
    combine(1)
    fake_step(1, df, 2, 1)
    fake_mate(2)
    combine(2)
    back_part(2)
    landed(px, px_recv)

    def turn_x(m, _):
        at = pl.ds(pl.multiple_of(m * chunk, chunk), chunk)
        own = pl.ds(pl.multiple_of(dp * wide + m * chunk, chunk), chunk)
        xo_t[at, :] = xf[:, own].T
        px_t[at, :] = px[:, at].T
        return 0

    lax.fori_loop(0, wide // chunk, turn_x, 0)
    fake_step(1, df, 3, 0)
    grad_down_part(2)
    combine(3)
    fake_step(1, df, 3, 1)
    fake_mate(3)
    combine(4)
    back_part(3)
    grad_down_part(3)
    combine(5)
    combine(6)
    fake_step(1, df, 4, 0)
    fake_step(1, df, 4, 1)
    fake_mate(4)
    back_part(4)
    remote(dpre, pdpre, dp_send.at[1], dp_recv.at[1], mate)
    grad_down_part(4)
    local(gd_ref, gd_hbm, o_sem.at[0])
    half = wide // 2
    for m in (0, 1):
        at = slice(m * half, (m + 1) * half)
        acc[at, :] = jnp.dot(xo_t[at, :], dpre[...], preferred_element_type=F32)
    combine(7)
    landed(pdpre, dp_recv.at[1])
    for m in (0, 1):
        at = slice(m * half, (m + 1) * half)
        gu_ref[at, :] = (
            acc[at, :] + jnp.dot(px_t[at, :], pdpre[...], preferred_element_type=F32)
        ).astype(BF)
        local(gu_ref.at[at, :], gu_hbm.at[at, :], o_sem.at[1 + m])
    landed(last, la_recv)
    out_ref[...] = (mine_f[...] + last[...].astype(F32)).astype(BF)
    local(out_ref, out_hbm, o_sem.at[3])

    most = pl.ds(0, (2 * nz - 1) * 128)
    seven = pl.ds(0, (ne - 1) * cap)
    landed(xt.at[:, most], xt_send)
    for i, src in enumerate((sx, sd)):
        landed(src.at[seven, :], fd_send.at[i, 0])
        landed(src, fd_send.at[i, 1])
    for i, ref in fakes:
        landed(ref.at[:, pl.ds(0, (2 * nz - 2) * 128)], f_send.at[i])
    landed(sent.at[seven, :], rd_send)
    landed(po.at[seven, :], rt_send)
    landed(cs.at[pl.ds(0, nz - 1)], rs_send)
    landed(last, la_send)
    landed(px, px_send)
    landed(pd, pd_send)
    landed(act_t, dp_send.at[0])
    landed(dpre, dp_send.at[1])
    landed(gd_ref, o_sem.at[0])
    for m in (0, 1):
        at = slice(m * half, (m + 1) * half)
        landed(gu_ref.at[at, :], o_sem.at[1 + m])
    landed(out_ref, o_sem.at[3])


def settle(*refs):
    count = 3
    given, kept, held = refs[:count], refs[count : 2 * count], refs[2 * count : 3 * count]
    get, put = refs[3 * count :]
    coming = [pltpu.make_async_copy(a, v, get.at[i]) for i, (a, v) in enumerate(zip(given, held))]
    going = [pltpu.make_async_copy(v, b, put.at[i]) for i, (v, b) in enumerate(zip(held, kept))]
    for copy in coming:
        copy.start()
    for first, then in zip(coming, going):
        first.wait()
        then.start()
    for copy in going:
        copy.wait()


def solution(mesh):
    ne, nt = mesh.shape["expert"], mesh.shape["tensor"]
    nz = nt // 2

    def on_device(
        x_real,
        routes_real,
        gates_real,
        up_real,
        down_real,
        x_fake,
        routes_fake,
        gates_fake,
        cotangent,
        up_fake,
        down_fake,
    ):
        tokens, part = x_real.shape
        cap = tokens // 2
        total = ne * cap
        width = up_real.shape[1]
        ff = up_real.shape[2]
        half = width // 2
        vmem = pl.BlockSpec(memory_space=pltpu.VMEM)
        hbm = pl.BlockSpec(memory_space=pl.ANY)
        dma = pltpu.SemaphoreType.DMA
        shapes = (
            jax.ShapeDtypeStruct((tokens, part), BF),
            jax.ShapeDtypeStruct((half, ff), BF),
            jax.ShapeDtypeStruct((ff, half), BF),
        )
        results = pl.pallas_call(
            functools.partial(kernel, (ne, nz, cap)),
            out_shape=shapes,
            in_specs=[vmem] * 7 + [hbm] * 4,
            out_specs=(hbm, hbm, hbm),
            scratch_shapes=[
                pltpu.VMEM((tokens, part), BF),
                pltpu.VMEM((half, ff), BF),
                pltpu.VMEM((ff, half), BF),
                pltpu.VMEM((half, total), BF),
                pltpu.VMEM((half, total), BF),
                pltpu.VMEM((width, ff), BF),
                pltpu.VMEM((ff, width), BF),
                pltpu.VMEM((width, ff), BF),
                pltpu.VMEM((ff, width), BF),
                pltpu.VMEM((total, tokens), BF),
                pltpu.VMEM((total, tokens), F32),
                pltpu.VMEM((tokens, total), BF),
                pltpu.VMEM((tokens, total), BF),
                pltpu.VMEM((total, part), BF),
                pltpu.VMEM((total, part), BF),
                pltpu.VMEM((tokens, width), BF),
                pltpu.VMEM((total, width), BF),
                pltpu.VMEM((total, width), BF),
                pltpu.VMEM((total, width), BF),
                pltpu.VMEM((total, width), BF),
                pltpu.VMEM((total, width), BF),
                pltpu.VMEM((total, width), BF),
                pltpu.VMEM((total, half), BF),
                pltpu.VMEM((total, half), BF),
                pltpu.VMEM((ff, total), BF),
                pltpu.VMEM((ff, total), BF),
                pltpu.VMEM((total, ff), BF),
                pltpu.VMEM((total, ff), BF),
                pltpu.VMEM((total, ff), F32),
                pltpu.VMEM((total, ff), F32),
                pltpu.VMEM((total, ff), BF),
                pltpu.VMEM((nz, tokens, 2 * part), BF),
                pltpu.VMEM((2, nz // 2, tokens, 2 * part), BF),
                pltpu.VMEM((tokens, part), F32),
                pltpu.VMEM((tokens, part), BF),
                dma((4,)),
                dma((4,)),
                dma,
                dma,
                dma,
                dma((2, nz // 2, 2)),
                dma((2, 2)),
                dma((2, 2)),
                dma((2,)),
                dma((2, 2, nz // 2, 2)),
                dma,
                dma((nz // 2 + 1, 2, 2)),
                dma((nz // 2 + 1, 2, 2)),
                dma,
                dma((nz, 2)),
                dma((2, 2, 2)),
                dma,
                dma((2, nz // 2)),
                dma,
                dma,
                dma,
                dma,
                dma,
                dma((nz // 2 + 1, 2)),
                dma((2,)),
                dma((2,)),
            ],
            compiler_params=pltpu.CompilerParams(
                collective_id=0, has_side_effects=True, vmem_limit_bytes=62 * 1024 * 1024
            ),
        )(
            x_real,
            x_fake,
            cotangent,
            routes_real.T,
            gates_real.T,
            routes_fake.T,
            gates_fake.T,
            up_real[0],
            down_real[0],
            up_fake[0],
            down_fake[0],
        )
        real_out, grad_up, grad_down = pl.pallas_call(
            settle,
            out_shape=shapes,
            in_specs=[hbm] * 3,
            out_specs=(hbm,) * 3,
            scratch_shapes=[pltpu.VMEM(a.shape, a.dtype) for a in shapes] + [dma((3,)), dma((3,))],
        )(*results)
        return real_out, grad_up[None], grad_down[None]

    placed = (
        P(("expert", "dp"), "tensor"),
        P(("expert", "dp"), None),
        P(("expert", "dp"), None),
        P("expert", None, "tensor"),
        P("expert", "tensor", None),
        P(("expert", "dp"), "tensor"),
        P(("expert", "dp"), None),
        P(("expert", "dp"), None),
        P(("expert", "dp"), "tensor"),
        P("expert", None, "tensor"),
        P("expert", "tensor", None),
    )
    return jax.shard_map(
        on_device,
        mesh=mesh,
        in_specs=placed,
        out_specs=(
            P(("expert", "dp"), "tensor"),
            P("expert", "dp", "tensor"),
            P("expert", "tensor", "dp"),
        ),
        check_vma=False,
    )
```

```python
import functools

import jax
import jax.numpy as jnp
from jax import lax
from jax.experimental import pallas as pl
from jax.experimental.pallas import tpu as pltpu
from jax.sharding import PartitionSpec as P

MESH = pl.DeviceIdType.MESH
BF = jnp.bfloat16
F32 = jnp.float32

slope_const = 0.7978845608028654
cubic_coef = 0.044715


def gelu_tanh(value):
    return (
        0.5 * value * (1.0 + jnp.tanh(slope_const * (value + cubic_coef * value * value * value)))
    )


def gelu_both(value):
    square = value * value
    inner = jnp.tanh(slope_const * (value + cubic_coef * square * value))
    act = 0.5 * value * (1.0 + inner)
    slope = 0.5 * (1.0 + inner) + 0.5 * value * (1.0 - inner * inner) * slope_const * (
        1.0 + 3.0 * cubic_coef * square
    )
    return act, slope


def over_rows(left, right):
    return lax.dot_general(left, right, (((0,), (0,)), ((), ())), preferred_element_type=F32)


def kernel(
    sizes,
    xr_in,
    xk_in,
    ct_in,
    rr_in,
    gr_in,
    rf_in,
    gf_in,
    wru_hbm,
    wrd_hbm,
    wfu_hbm,
    wfd_hbm,
    out_hbm,
    gu_hbm,
    gd_hbm,
    out_ref,
    gu_ref,
    gd_ref,
    xo_t,
    px_t,
    xr_ref,
    xk_ref,
    ct_ref,
    rr_ref,
    gr_ref,
    rf_ref,
    gf_ref,
    wru,
    wrd,
    wfu,
    wfd,
    spread,
    wt,
    high,
    low,
    sx,
    sd,
    xt,
    sent,
    rows,
    po,
    ret,
    xf,
    df,
    px,
    pd,
    act_t,
    pact_t,
    dpre,
    pdpre,
    slope,
    acc,
    hidden,
    cs,
    rs,
    mine_f,
    last,
    w_sem,
    o_sem,
    i_sem,
    loc_sem,
    xt_send,
    xt_yh,
    xt_recv,
    fd_send,
    fd_recv,
    f_send,
    f_recv,
    rd_send,
    rd_recv,
    rh_recv,
    rt_send,
    rt_recv,
    rth_recv,
    rs_send,
    rs_recv,
    la_send,
    la_recv,
    px_send,
    px_recv,
    pd_send,
    pd_recv,
    dp_send,
    dp_recv,
):
    ne, nz, cap = sizes
    e = lax.axis_index("expert")
    t = lax.axis_index("tensor")
    dp = lax.axis_index("dp")
    yh = t // nz
    z = t % nz
    oy = 1 - yh
    wide = nz * 128
    total = ne * cap

    def near(step):
        return (z + step + nz) % nz

    def cols(zz, sub):
        y = yh if sub == 0 else oy
        return pl.ds(pl.multiple_of(y * wide + zz * 128, 128), 128)

    def block(expert):
        return pl.ds(pl.multiple_of(expert * cap, cap), cap)

    def remote(src, dst, send, recv, where):
        pltpu.make_async_remote_copy(
            src_ref=src, dst_ref=dst, send_sem=send, recv_sem=recv, device_id=where, device_id_type=MESH
        ).start()

    def local(src, dst, sem):
        pltpu.make_async_copy(src, dst, sem).start()

    def landed(ref, sem):
        pltpu.make_async_copy(ref, ref, sem).wait()

    other = (e, oy * nz + z, dp)
    mate = (e, t, 1 - dp)
    sides = ((e, yh * nz + near(1), dp), (e, yh * nz + near(-1), dp))

    inputs = (
        (xr_in, xr_ref),
        (xk_in, xk_ref),
        (ct_in, ct_ref),
        (rr_in, rr_ref),
        (gr_in, gr_ref),
        (rf_in, rf_ref),
        (gf_in, gf_ref),
    )
    for i, (src, dst) in enumerate(inputs):
        local(src, dst, i_sem.at[i])
    barrier = pltpu.get_barrier_semaphore()

    def greet_expert(k, _):
        for y in (yh, oy):
            pl.semaphore_signal(
                barrier, inc=1, device_id=((e + k) % ne, y * nz + z, dp), device_id_type=MESH
            )
        return 0

    lax.fori_loop(1, ne, greet_expert, 0)
    for peer in (*sides, other):
        pl.semaphore_signal(barrier, inc=1, device_id=peer, device_id_type=MESH)
    pl.semaphore_signal(barrier, inc=1, device_id=mate, device_id_type=MESH)
    for i, (src, dst) in enumerate(inputs):
        pltpu.make_async_copy(src, dst, i_sem.at[i]).wait()
    local(xr_ref, xt.at[:, cols(z, 0)], loc_sem)
    for i, (src, dst) in enumerate(((wru_hbm, wru), (wrd_hbm, wrd), (wfu_hbm, wfu), (wfd_hbm, wfd))):
        local(src, dst, w_sem.at[i])

    tokens = xr_ref.shape[0]
    chunk = 256
    earlier = (
        lax.broadcasted_iota(jnp.int32, (tokens, tokens), 0)
        < lax.broadcasted_iota(jnp.int32, (tokens, tokens), 1)
    ).astype(F32).astype(BF)
    labels = lax.broadcasted_iota(jnp.int32, (2 * ne, tokens), 0)

    def places(routes):
        hits = [(labels == routes[k : k + 1, :]).astype(F32) for k in (0, 1)]
        before = jnp.dot(
            (hits[0] + hits[1]).astype(BF), earlier, preferred_element_type=F32
        )
        return [
            routes[k : k + 1, :] * cap
            + jnp.sum(hits[k] * before, axis=0, keepdims=True).astype(jnp.int32)
            for k in (0, 1)
        ]

    def matches(at, places_of):
        slots = at * chunk + lax.broadcasted_iota(jnp.int32, (chunk, tokens), 0)
        return [slots == p for p in places_of]

    def weigh(masks, gates):
        return jnp.where(masks[0], gates[0:1, :], 0.0) + jnp.where(masks[1], gates[1:2, :], 0.0)

    fake_places = places(rf_ref[...])

    def fake_slots(r, _):
        at = pl.ds(pl.multiple_of(r * chunk, chunk), chunk)
        masks = matches(r, fake_places)
        pick = (masks[0] | masks[1]).astype(F32).astype(BF)
        sx[at, :] = jnp.dot(pick, xk_ref[...], preferred_element_type=F32).astype(BF)
        gate = jnp.sum(weigh(masks, gf_ref[...]), axis=1, keepdims=True)
        sd[at, :] = (gate * jnp.dot(pick, ct_ref[...], preferred_element_type=F32)).astype(BF)
        return 0

    lax.fori_loop(0, total // chunk, fake_slots, 0)
    real_places = places(rr_ref[...])

    def real_slots(r, _):
        at = pl.ds(pl.multiple_of(r * chunk, chunk), chunk)
        masks = matches(r, real_places)
        spread[at, :] = (masks[0] | masks[1]).astype(F32).astype(BF)
        wt[at, :] = weigh(masks, gr_ref[...])
        return 0

    lax.fori_loop(0, total // chunk, real_slots, 0)
    pl.semaphore_wait(barrier, 2 * (ne - 1) + 4)

    def ring_send(ref, zz, sub, way, dist, send, recv):
        remote(
            ref.at[:, cols(zz, sub)],
            ref.at[:, cols(zz, sub)],
            send,
            recv.at[way, dist - 1, sub],
            sides[way],
        )

    def ring_take(ref, dist, sub, send, recv):
        for way in (0, 1):
            if dist == nz // 2 and way != sub:
                continue
            zz = near(-dist if way == 0 else dist)
            landed(ref.at[:, cols(zz, sub)], recv.at[way, dist - 1, sub])
            if dist < nz // 2 - 1 or (dist == nz // 2 - 1 and way == sub):
                ring_send(ref, zz, sub, way, dist + 1, send, recv)

    local_x = pltpu.make_async_copy(xr_ref, xt.at[:, cols(z, 0)], loc_sem)
    local_x.wait()
    for way in (0, 1):
        ring_send(xt, z, 0, way, 1, xt_send, xt_recv)
    remote(xt.at[:, cols(z, 0)], xt.at[:, cols(z, 0)], xt_send, xt_yh, other)

    def fake_give(i, src, dst, far):
        y = oy if far else yh

        def give(k, _):
            to = (e + k) % ne
            remote(
                src.at[block(to), :],
                dst.at[block(e), cols(z, 0)],
                fd_send.at[i, far],
                fd_recv.at[i, far],
                (to, y * nz + z, dp),
            )
            return 0

        lax.fori_loop(1 - far, ne, give, 0)
        if not far:
            local(src.at[block(e), :], dst.at[block(e), cols(z, 0)], fd_recv.at[i, 0])

    fake_give(0, sx, xf, 0)

    def slot(zz, sub):
        sent[:, cols(zz, sub)] = jnp.dot(
            spread[...], xt[:, cols(zz, sub)], preferred_element_type=F32
        ).astype(BF)

    def pair_of(dist):
        return (near(dist),) if dist in (0, nz // 2) else (near(-dist), near(dist))

    def share(expert, part):
        if part is None:
            return block(expert)
        return pl.ds(pl.multiple_of(expert * cap + part * (cap // 2), cap // 2), cap // 2)

    late = (2, 3, 4)
    flip = e + 1 - 2 * (e % 2)

    def dispatch(dist, sub, part=None):
        def send(at, to, y, part, recv):
            remote(
                sent.at[share(to, part), at], rows.at[share(e, part), at], rd_send, recv, (to, y * nz + z, dp)
            )

        for n, zz in enumerate(pair_of(dist)):
            at = cols(zz, sub)
            recv = rd_recv.at[dist, n, sub] if part is None else rh_recv.at[dist, n, part]

            def along(k, _, at=at, recv=recv):
                send(at, (e + 2 * k) % ne, yh, part, recv)
                return 0

            lax.fori_loop(1, ne // 2, along, 0)
            local(sent.at[share(e, part), at], rows.at[share(e, part), at], recv)
            if sub == 0:

                def across(k, _, at=at, recv=recv, n=n):
                    to = (flip + 2 * k) % ne
                    send(at, to, yh, None, recv)
                    if dist in late:
                        for half in (0, 1):
                            send(at, to, oy, half, rh_recv.at[dist, n, half])
                    else:
                        send(at, to, oy, None, rd_recv.at[dist, n, 1])
                    return 0

                lax.fori_loop(0, ne // 2, across, 0)

    def real_step(dist, sub):
        ring_take(xt, dist, sub, xt_send, xt_recv)
        for zz in pair_of(dist):
            slot(zz, sub)
        dispatch(dist, sub, 0 if sub == 1 and dist in late else None)

    def up_part(dist, sub):
        where = [cols(zz, sub) for zz in pair_of(dist)]
        for n, zz in enumerate(pair_of(dist)):
            landed(rows.at[:, cols(zz, sub)], rd_recv.at[dist, n, sub])
        w = jnp.concatenate([wru[c, :] for c in where], axis=0)

        def part(r, _):
            at = pl.ds(pl.multiple_of(r * chunk, chunk), chunk)
            got = jnp.concatenate([rows[at, c] for c in where], axis=1)
            pre = jnp.dot(got, w, preferred_element_type=F32)
            if dist == 0 and sub == 0:
                acc[at, :] = pre
            else:
                acc[at, :] += pre
            return 0

        lax.fori_loop(0, total // chunk, part, 0)

    def halves(r, part):
        return [share(r * 4 + j, part) for j in range(4)]

    def up_half(part):
        where = [cols(zz, 1) for dist in late for zz in pair_of(dist)]
        for dist in late:
            for n, zz in enumerate(pair_of(dist)):
                half_bytes = rows.at[pl.ds(0, total // 2), cols(zz, 1)]
                landed(half_bytes, rh_recv.at[dist, n, part])
        w = jnp.concatenate([wru[c, :] for c in where], axis=0)

        def some(r, _):
            ats = halves(r, part)
            got = jnp.concatenate(
                [jnp.concatenate([rows[at, c] for c in where], axis=1) for at in ats], axis=0
            )
            pre = jnp.dot(got, w, preferred_element_type=F32)
            for j, at in enumerate(ats):
                own = acc[at, :] + pre[j * (cap // 2) : (j + 1) * (cap // 2), :]
                hidden[at, :] = gelu_tanh(own).astype(BF)
            return 0

        lax.fori_loop(0, ne // 4, some, 0)

    fakes = ((0, xf), (1, df))

    def fake_own(i, ref, sub):
        landed(ref.at[:, cols(z, sub)], fd_recv.at[i, sub])
        for way in (0, 1):
            ring_send(ref, z, sub, way, 1, f_send.at[i], f_recv.at[i])

    def fake_step(i, ref, dist, sub):
        ring_take(ref, dist, sub, f_send.at[i], f_recv.at[i])

    def fake_up(r, _):
        at = pl.ds(pl.multiple_of(r * chunk, chunk), chunk)
        pre = jnp.dot(xf[at, :], wfu[...], preferred_element_type=F32)
        a, s = gelu_both(pre)
        act_t[:, at] = a.T.astype(BF)
        slope[at, :] = s
        return 0

    theirs = pl.ds(pl.multiple_of((1 - dp) * wide, 128), wide)

    slot(z, 0)
    dispatch(0, 0)
    real_step(1, 0)
    fake_give(0, sx, xf, 1)
    real_step(2, 0)
    fake_own(0, xf, 0)
    real_step(3, 0)
    landed(xt.at[:, cols(z, 1)], xt_yh)
    for way in (0, 1):
        ring_send(xt, z, 1, way, 1, xt_send, xt_recv)
    slot(z, 1)
    dispatch(0, 1)
    real_step(1, 1)
    real_step(4, 0)
    fake_own(0, xf, 1)
    real_step(2, 1)
    fake_step(0, xf, 1, 0)
    fake_give(1, sd, df, 0)
    fake_give(1, sd, df, 1)
    real_step(3, 1)
    real_step(4, 1)
    for dist in late:
        dispatch(dist, 1, 1)
    weights = wt[...].T
    rounded = weights.astype(BF)
    high[...] = rounded
    low[...] = (weights - rounded.astype(F32)).astype(BF)
    for i, (src, dst) in enumerate(((wru_hbm, wru), (wrd_hbm, wrd), (wfu_hbm, wfu), (wfd_hbm, wfd))):
        pltpu.make_async_copy(src, dst, w_sem.at[i]).wait()
    up_part(0, 0)
    up_part(1, 0)
    fake_step(0, xf, 1, 1)
    up_part(2, 0)
    fake_step(0, xf, 2, 0)
    up_part(3, 0)
    up_part(4, 0)
    up_part(0, 1)
    fake_step(0, xf, 2, 1)
    up_part(1, 1)
    fake_step(0, xf, 3, 0)
    fake_own(1, df, 0)
    fake_own(1, df, 1)
    up_half(0)

    early = (0, 1)
    turns = [nz // 2] + [way * d for d in range(nz // 2 - 1, 0, -1) for way in (-1, 1)] + [0]

    def down(step, part=None):
        zz = near(turns[step])
        w = jnp.concatenate([wrd[:, cols(zz, 0)], wrd[:, cols(zz, 1)]], axis=1)

        def some(r, _):
            if part is None:
                ats = [pl.ds(pl.multiple_of(r * chunk, chunk), chunk)]
            else:
                ats = halves(r, part)
            got = [hidden[at, :] for at in ats]
            got = got[0] if part is None else jnp.concatenate(got, axis=0)
            got = jnp.dot(got, w, preferred_element_type=F32).astype(BF)
            size = chunk // len(ats)
            for j, at in enumerate(ats):
                po[at, cols(zz, 0)] = got[j * size : (j + 1) * size, :128]
                po[at, cols(zz, 1)] = got[j * size : (j + 1) * size, 128:]
            return 0

        lax.fori_loop(0, total // chunk if part is None else ne // 4, some, 0)

    def give_back(step, part=None):
        zz = near(turns[step])
        for sub in (0, 1):

            def recv(sub):
                return rt_recv.at[step, sub] if part is None else rth_recv.at[step, sub, part]

            def send(to, y, sub, into):
                remote(
                    po.at[share(to, part), cols(zz, sub)],
                    ret.at[share(e, part), cols(zz, sub)],
                    rt_send,
                    recv(into),
                    (to, y * nz + z, dp),
                )

            def along(k, _, sub=sub):
                send((e + 2 * k) % ne, yh, sub, sub)
                return 0

            def across(k, _, sub=sub):
                to = (flip + 2 * k) % ne
                if step % 2 == 0:
                    send(to, yh, sub, sub)
                else:
                    send(to, oy, sub, 1 - sub)
                return 0

            lax.fori_loop(1, ne // 2, along, 0)
            lax.fori_loop(0, ne // 2, across, 0)
            local(
                po.at[share(e, part), cols(zz, sub)], ret.at[share(e, part), cols(zz, sub)], recv(sub)
            )

    for step in early:
        down(step, 0)
    for step in early:
        give_back(step, 0)
    fake_step(0, xf, 3, 1)
    up_half(1)
    for step in early:
        down(step, 1)
    for step in early:
        give_back(step, 1)
    down(len(early))
    for step in range(len(early) + 1, nz):
        down(step)
        give_back(step - 1)
    give_back(nz - 1)

    def combine(step):
        turn = turns[step]
        dist = abs(turn)
        zz = near(turn)
        for sub in (0, 1):
            if step in early:
                for part in (0, 1):
                    landed(ret.at[pl.ds(0, total // 2), cols(zz, sub)], rth_recv.at[step, sub, part])
            else:
                landed(ret.at[:, cols(zz, sub)], rt_recv.at[step, sub])
        got = jnp.concatenate([ret[:, cols(zz, 0)], ret[:, cols(zz, 1)]], axis=1)
        both = jnp.dot(high[...], got, preferred_element_type=F32) + jnp.dot(
            low[...], got, preferred_element_type=F32
        )
        left, right = pl.ds(0, 128), pl.ds(128, 128)
        if dist == nz // 2:
            cs[step] = both.astype(BF)
            for way, half in ((0, left), (1, right)):
                remote(
                    cs.at[step, :, half],
                    rs.at[way, dist - 1, :, half],
                    rs_send,
                    rs_recv.at[way, dist - 1],
                    sides[way],
                )
        elif dist > 0:
            way = 0 if turn > 0 else 1
            if dist == nz // 2 - 1:
                half = (left, right)[way]
                landed(rs.at[way, dist, :, half], rs_recv.at[way, dist])
                cs[step] = both.astype(BF)
                more = both[:, way * 128 : (way + 1) * 128] + rs[way, dist, :, half].astype(F32)
                cs[step, :, half] = more.astype(BF)
            else:
                landed(rs.at[way, dist], rs_recv.at[way, dist])
                cs[step] = (both + rs[way, dist].astype(F32)).astype(BF)
            remote(
                cs.at[step], rs.at[way, dist - 1], rs_send, rs_recv.at[way, dist - 1], sides[way]
            )
        else:
            for way in (0, 1):
                landed(rs.at[way, 0], rs_recv.at[way, 0])
            both = both + rs[0, 0].astype(F32) + rs[1, 0].astype(F32)
            mine_f[...] = both[:, :128]
            cs[step, :, right] = both[:, 128:].astype(BF)
            remote(cs.at[step, :, right], last, la_send, la_recv, other)

    def half_cols(zz, side):
        return pl.ds(pl.multiple_of(side * wide + zz * 128, 128), 128)

    def fake_mate(dist):
        for n, zz in enumerate(pair_of(dist)):
            at = pl.ds(pl.multiple_of(zz * 128, 128), 128)
            remote(df.at[:, half_cols(zz, 1 - dp)], pd.at[:, at], pd_send, pd_recv.at[dist, n], mate)

    def back_part(dist):
        for zz in pair_of(dist):
            w = jnp.concatenate([wfd[:, cols(zz, 0)], wfd[:, cols(zz, 1)]], axis=1)

            def part(r, _, zz=zz, w=w):
                at = pl.ds(pl.multiple_of(r * chunk, chunk), chunk)
                rows_d = jnp.concatenate([df[at, cols(zz, 0)], df[at, cols(zz, 1)]], axis=1)
                back = lax.dot_general(
                    rows_d, w, (((1,), (1,)), ((), ())), preferred_element_type=F32
                )
                if dist == 0:
                    acc[at, :] = back
                elif dist == nz // 2:
                    dpre[at, :] = ((acc[at, :] + back) * slope[at, :]).astype(BF)
                else:
                    acc[at, :] += back
                return 0

            lax.fori_loop(0, total // chunk, part, 0)

    def grad_down_part(dist):
        zs = pair_of(dist)
        ats = [pl.ds(pl.multiple_of(zz * 128, 128), 128) for zz in zs]
        for n, at in enumerate(ats):
            landed(pd.at[:, at], pd_recv.at[dist, n])
        own = [df[:, half_cols(zz, dp)] for zz in zs]
        got = [pd[:, at] for at in ats]
        if len(zs) == 2:
            own, got = [jnp.concatenate(own, axis=1)], [jnp.concatenate(got, axis=1)]
        grad = jnp.dot(act_t[...], own[0], preferred_element_type=F32) + jnp.dot(
            pact_t[...], got[0], preferred_element_type=F32
        )
        grad = grad.astype(BF)
        for n, at in enumerate(ats):
            gd_ref[:, at] = grad[:, n * 128 : (n + 1) * 128]

    fake_step(1, df, 1, 0)
    fake_step(0, xf, 4, 0)
    fake_step(0, xf, 4, 1)
    remote(xf.at[:, theirs], px, px_send, px_recv, mate)
    lax.fori_loop(0, total // chunk, fake_up, 0)
    fake_step(1, df, 1, 1)
    remote(act_t, pact_t, dp_send.at[0], dp_recv.at[0], mate)
    fake_mate(0)
    fake_mate(1)
    combine(0)
    back_part(0)
    back_part(1)
    landed(pact_t, dp_recv.at[0])
    fake_step(1, df, 2, 0)
    grad_down_part(0)
    grad_down_part(1)
    combine(1)
    fake_step(1, df, 2, 1)
    fake_mate(2)
    combine(2)
    back_part(2)
    landed(px, px_recv)

    def turn_x(m, _):
        at = pl.ds(pl.multiple_of(m * chunk, chunk), chunk)
        own = pl.ds(pl.multiple_of(dp * wide + m * chunk, chunk), chunk)
        xo_t[at, :] = xf[:, own].T
        px_t[at, :] = px[:, at].T
        return 0

    lax.fori_loop(0, wide // chunk, turn_x, 0)
    fake_step(1, df, 3, 0)
    grad_down_part(2)
    combine(3)
    combine(4)
    fake_step(1, df, 3, 1)
    fake_mate(3)
    back_part(3)
    combine(5)
    grad_down_part(3)
    combine(6)
    fake_step(1, df, 4, 0)
    fake_step(1, df, 4, 1)
    fake_mate(4)
    back_part(4)
    remote(dpre, pdpre, dp_send.at[1], dp_recv.at[1], mate)
    combine(7)
    grad_down_part(4)
    local(gd_ref, gd_hbm, o_sem.at[0])
    half = wide // 2
    for m in (0, 1):
        at = slice(m * half, (m + 1) * half)
        acc[at, :] = jnp.dot(xo_t[at, :], dpre[...], preferred_element_type=F32)
    landed(pdpre, dp_recv.at[1])
    for m in (0, 1):
        at = slice(m * half, (m + 1) * half)
        gu_ref[at, :] = (
            acc[at, :] + jnp.dot(px_t[at, :], pdpre[...], preferred_element_type=F32)
        ).astype(BF)
        local(gu_ref.at[at, :], gu_hbm.at[at, :], o_sem.at[1 + m])
    landed(last, la_recv)
    out_ref[...] = (mine_f[...] + last[...].astype(F32)).astype(BF)
    local(out_ref, out_hbm, o_sem.at[3])

    most = pl.ds(0, (2 * nz - 1) * 128)
    seven = pl.ds(0, (ne - 1) * cap)
    landed(xt.at[:, most], xt_send)
    for i, src in enumerate((sx, sd)):
        landed(src.at[seven, :], fd_send.at[i, 0])
        landed(src, fd_send.at[i, 1])
    for i, ref in fakes:
        landed(ref.at[:, pl.ds(0, (2 * nz - 2) * 128)], f_send.at[i])
    landed(sent.at[seven, :], rd_send)
    landed(po.at[seven, :], rt_send)
    landed(cs.at[pl.ds(0, nz - 1)], rs_send)
    landed(last, la_send)
    landed(px, px_send)
    landed(pd, pd_send)
    landed(act_t, dp_send.at[0])
    landed(dpre, dp_send.at[1])
    landed(gd_ref, o_sem.at[0])
    for m in (0, 1):
        at = slice(m * half, (m + 1) * half)
        landed(gu_ref.at[at, :], o_sem.at[1 + m])
    landed(out_ref, o_sem.at[3])


def settle(*refs):
    count = 3
    given, kept, held = refs[:count], refs[count : 2 * count], refs[2 * count : 3 * count]
    get, put = refs[3 * count :]
    coming = [pltpu.make_async_copy(a, v, get.at[i]) for i, (a, v) in enumerate(zip(given, held))]
    going = [pltpu.make_async_copy(v, b, put.at[i]) for i, (v, b) in enumerate(zip(held, kept))]
    for copy in coming:
        copy.start()
    for first, then in zip(coming, going):
        first.wait()
        then.start()
    for copy in going:
        copy.wait()


def solution(mesh):
    ne, nt = mesh.shape["expert"], mesh.shape["tensor"]
    nz = nt // 2

    def on_device(
        x_real,
        routes_real,
        gates_real,
        up_real,
        down_real,
        x_fake,
        routes_fake,
        gates_fake,
        cotangent,
        up_fake,
        down_fake,
    ):
        tokens, part = x_real.shape
        cap = tokens // 2
        total = ne * cap
        width = up_real.shape[1]
        ff = up_real.shape[2]
        half = width // 2
        hbm = pl.BlockSpec(memory_space=pl.ANY)
        dma = pltpu.SemaphoreType.DMA
        shapes = (
            jax.ShapeDtypeStruct((tokens, part), BF),
            jax.ShapeDtypeStruct((half, ff), BF),
            jax.ShapeDtypeStruct((ff, half), BF),
        )
        results = pl.pallas_call(
            functools.partial(kernel, (ne, nz, cap)),
            out_shape=shapes,
            in_specs=[hbm] * 11,
            out_specs=(hbm, hbm, hbm),
            scratch_shapes=[
                pltpu.VMEM((tokens, part), BF),
                pltpu.VMEM((half, ff), BF),
                pltpu.VMEM((ff, half), BF),
                pltpu.VMEM((half, total), BF),
                pltpu.VMEM((half, total), BF),
                pltpu.VMEM((tokens, part), BF),
                pltpu.VMEM((tokens, part), BF),
                pltpu.VMEM((tokens, part), BF),
                pltpu.VMEM((2, tokens), jnp.int32),
                pltpu.VMEM((2, tokens), F32),
                pltpu.VMEM((2, tokens), jnp.int32),
                pltpu.VMEM((2, tokens), F32),
                pltpu.VMEM((width, ff), BF),
                pltpu.VMEM((ff, width), BF),
                pltpu.VMEM((width, ff), BF),
                pltpu.VMEM((ff, width), BF),
                pltpu.VMEM((total, tokens), BF),
                pltpu.VMEM((total, tokens), F32),
                pltpu.VMEM((tokens, total), BF),
                pltpu.VMEM((tokens, total), BF),
                pltpu.VMEM((total, part), BF),
                pltpu.VMEM((total, part), BF),
                pltpu.VMEM((tokens, width), BF),
                pltpu.VMEM((total, width), BF),
                pltpu.VMEM((total, width), BF),
                pltpu.VMEM((total, width), BF),
                pltpu.VMEM((total, width), BF),
                pltpu.VMEM((total, width), BF),
                pltpu.VMEM((total, width), BF),
                pltpu.VMEM((total, half), BF),
                pltpu.VMEM((total, half), BF),
                pltpu.VMEM((ff, total), BF),
                pltpu.VMEM((ff, total), BF),
                pltpu.VMEM((total, ff), BF),
                pltpu.VMEM((total, ff), BF),
                pltpu.VMEM((total, ff), F32),
                pltpu.VMEM((total, ff), F32),
                pltpu.VMEM((total, ff), BF),
                pltpu.VMEM((nz, tokens, 2 * part), BF),
                pltpu.VMEM((2, nz // 2, tokens, 2 * part), BF),
                pltpu.VMEM((tokens, part), F32),
                pltpu.VMEM((tokens, part), BF),
                dma((4,)),
                dma((4,)),
                dma((7,)),
                dma,
                dma,
                dma,
                dma((2, nz // 2, 2)),
                dma((2, 2)),
                dma((2, 2)),
                dma((2,)),
                dma((2, 2, nz // 2, 2)),
                dma,
                dma((nz // 2 + 1, 2, 2)),
                dma((nz // 2 + 1, 2, 2)),
                dma,
                dma((nz, 2)),
                dma((2, 2, 2)),
                dma,
                dma((2, nz // 2)),
                dma,
                dma,
                dma,
                dma,
                dma,
                dma((nz // 2 + 1, 2)),
                dma((2,)),
                dma((2,)),
            ],
            compiler_params=pltpu.CompilerParams(
                collective_id=0, has_side_effects=True, vmem_limit_bytes=62 * 1024 * 1024
            ),
        )(
            x_real,
            x_fake,
            cotangent,
            routes_real.T,
            gates_real.T,
            routes_fake.T,
            gates_fake.T,
            up_real[0],
            down_real[0],
            up_fake[0],
            down_fake[0],
        )
        real_out, grad_up, grad_down = pl.pallas_call(
            settle,
            out_shape=shapes,
            in_specs=[hbm] * 3,
            out_specs=(hbm,) * 3,
            scratch_shapes=[pltpu.VMEM(a.shape, a.dtype) for a in shapes] + [dma((3,)), dma((3,))],
        )(*results)
        return real_out, grad_up[None], grad_down[None]

    placed = (
        P(("expert", "dp"), "tensor"),
        P(("expert", "dp"), None),
        P(("expert", "dp"), None),
        P("expert", None, "tensor"),
        P("expert", "tensor", None),
        P(("expert", "dp"), "tensor"),
        P(("expert", "dp"), None),
        P(("expert", "dp"), None),
        P(("expert", "dp"), "tensor"),
        P("expert", None, "tensor"),
        P("expert", "tensor", None),
    )
    return jax.shard_map(
        on_device,
        mesh=mesh,
        in_specs=placed,
        out_specs=(
            P(("expert", "dp"), "tensor"),
            P("expert", "dp", "tensor"),
            P("expert", "tensor", "dp"),
        ),
        check_vma=False,
    )
```
